128 devices in a mesh: dp: 8 (over z, y_hi), expert: 4 (over y_lo, core), sample: 4 (over x).
Axes of the slice: x: 4, y: 4 (y_hi: 2, y_lo: 2; y = y_hi * 2 + y_lo), z: 4, core: 2. Of those that a mesh axis runs over, the one named last changes fastest.
Arguments:
- tokens: bfloat16 [2560, 4096], P(('dp', 'expert', 'sample')), may hold values from -6 to 6
- cotangent: bfloat16 [2560, 4096], P(('dp', 'expert', 'sample')), may hold values from -6 to 6
- routes: int32 [2560, 2], P(('dp', 'expert', 'sample')), may hold values from 0 to 7, all different within a row; in each aligned block of 20 rows (0 to 19, 20 to 39, ...) at most 6 rows name the same one
- gate_weights: float32 [2560, 2], P(('dp', 'expert', 'sample')), may hold values from 0.1 to 1
- lengths: int32 [32, 4], P(('dp', 'expert'), 'sample'), may hold values from 1 to 20
- rewards: int32 [32, 4], P(('dp', 'expert'), 'sample'), may hold values from -48 to 48
- w_gate: bfloat16 [8, 8192, 4096], P('expert', ('dp', 'sample')), may hold values from -0.09375 to 0.09375
- w_up: bfloat16 [8, 8192, 4096], P('expert', ('dp', 'sample')), may hold values from -0.09375 to 0.09375
- w_down: bfloat16 [8, 8192, 4096], P('expert', ('dp', 'sample')), may hold values from -0.0625 to 0.0625
Outputs:
- grad_tokens: bfloat16 [2560, 4096], P(('dp', 'expert', 'sample'))
- grad_w_gate: bfloat16 [8, 8192, 4096], P('expert', ('dp', 'sample'))
- grad_w_up: bfloat16 [8, 8192, 4096], P('expert', ('dp', 'sample'))
- grad_w_down: bfloat16 [8, 8192, 4096], P('expert', ('dp', 'sample'))
The draws below stay inside these ranges and needn't reach their ends.
Inputs may be any that keep to these rules, and one draw needn't show every extreme that they name: `routes`: each row names 2 different experts; among the rows of one device no expert is named by more than 6 rows, and in every draw some device's rows name some expert exactly 6 times.
All inputs are finite; a program needn't handle non-finite values.
Results may differ from the reference program's by a relative error of at most 0.025.
Values may be sent and summed in bfloat16 or wider, within the bound.
A program may use at most 192 MiB of HBM per device.

```python
import math
import jax
import jax.numpy as jnp
import numpy as np
from jax import lax

D = 4096
FF = 8192
EXPERTS = 8
TOP = 2
TOK_DEV = 20
CAP = 6
K = 4
PROMPTS = 32
TOKENS = 2560
N_DP = 8
N_EXPERT = 4
N_SAMPLE = 4


def touch_ends(drawn, rng, low, top_value):
    longest = drawn.shape.index(max(drawn.shape))
    spots = []
    for shift in (0, 1):
        where = [jax.random.randint(jax.random.fold_in(rng, axis), (), 0, length) for axis, length in enumerate(drawn.shape)]
        where[longest] = (where[longest] + shift) % drawn.shape[longest]
        spots.append(tuple(where))
    return drawn.at[spots[0]].set(low).at[spots[1]].set(top_value)


def block_scale(rng, shape, pieces, smallest, top_value):
    def one(dim, parts):
        heights = jax.random.uniform(jax.random.fold_in(jax.random.fold_in(rng, 6), dim), (parts,), jnp.float32, smallest / len(pieces), top_value / len(pieces))
        return jnp.repeat(jnp.exp(heights), shape[dim] // parts).reshape((-1,) + (1,) * (len(shape) - dim - 1))

    loudness = one(*pieces[0])
    for cut in pieces[1:]:
        loudness = loudness * one(*cut)
    return loudness


def shared_out(rng, own, number, rows, count, top, most, skew):
    ranking = jax.random.permutation(rng, count)
    crowded, usual = portions_of(count, rows * top, most, skew, True), portions_of(count, rows * top, most, skew, False)
    places = jnp.arange(count)

    def named(sizes, offset_by):
        used = int((sizes > 0).sum())
        fixed = max(1, used // 4)
        passed = fixed + (places - fixed + offset_by * (used - fixed)) % max(1, count - fixed)
        return jnp.zeros((count,), jnp.int32).at[ranking[jnp.where(places < fixed, places, passed)]].set(jnp.asarray(sizes, jnp.int32))

    sizes = jnp.where(number % 4 == 0, named(crowded, number // 4), named(usual, number - number // 4 - 1))
    mixed = jax.random.permutation(jax.random.fold_in(own, 3), count)
    giver, receiver = mixed[0:count // 2 * 2:2], mixed[1:count // 2 * 2:2]
    margin = jnp.minimum(sizes[giver] - 1, most - sizes[receiver]) // 2
    margin = jnp.where((giver == ranking[0]) | (receiver == ranking[0]) | (sizes[receiver] == 0), 0, jnp.maximum(margin, 0))
    passed = jax.random.randint(jax.random.fold_in(own, 4), (count // 2,), 0, 1 << 20) % (margin + 1)
    sizes = sizes.at[giver].add(-passed).at[receiver].add(passed)
    labels = jnp.searchsorted(jnp.cumsum(sizes), jnp.arange(rows * top), side="right").astype(jnp.int32)
    grid = labels.reshape(top, rows).T
    grid = grid[jax.random.permutation(jax.random.fold_in(own, 1), rows)]
    offset_by = jax.random.randint(jax.random.fold_in(own, 2), (rows, 1), 0, top)
    return jnp.take_along_axis(grid, (jnp.arange(top)[None, :] + offset_by) % top, axis=1)


def portions_of(amount, total, bound, skew, full):
    weights = [(1 << 20) // math.isqrt(standing ** skew) + 1 for standing in range(1, amount + 1)]
    largest = bound if full else min(bound, max(-(-total // amount), total * weights[0] // sum(weights)))
    least = 1 if total - largest >= amount - 1 else 0
    holding, spare = [largest] + [least] * (amount - 1), total - largest - least * (amount - 1)
    while spare > 0:
        candidates = [i for i in range(1, amount) if holding[i] < largest] or [i for i in range(1, amount) if holding[i] < bound]
        whole, budget = sum([weights[i] for i in candidates]), spare
        for i in candidates:
            more = min(bound - holding[i], max(1, budget * weights[i] // whole), spare)
            holding[i] = holding[i] + more
            spare = spare - more
    return np.array(holding)


def centred(key, dims, spread, reach, shards=(), kind=jnp.bfloat16):
    gain = block_scale(key, dims, shards, -0.22, 0.18) if shards else 1.0
    array = jax.random.normal(key, dims, jnp.float32) * spread * gain
    return jnp.minimum(jnp.maximum(array, -reach), reach).astype(kind)


def setup_inputs(seed: int = 0) -> dict:
    streams_of = jax.random.split(jax.random.key(seed), 10)
    tokens = centred(streams_of[0], (TOKENS, D), 1.0, 6.0, ((0, 128),))
    cotangent = centred(streams_of[1], (TOKENS, D), 1.0, 6.0, ((0, 128),))
    routes_keys = jax.random.split(jax.random.fold_in(streams_of[2], 1), TOKENS // TOK_DEV)
    routes_turns = jax.random.permutation(jax.random.fold_in(streams_of[2], 3), TOKENS // TOK_DEV)
    routes = jax.vmap(lambda own, number: shared_out(jax.random.fold_in(streams_of[2], 2), own, number, TOK_DEV, EXPERTS, TOP, CAP, 2))(routes_keys, routes_turns).reshape((TOKENS, TOP))
    gate_weights = jnp.clip(0.1 + 0.9 * jax.random.uniform(streams_of[3], (TOKENS, TOP), jnp.float32) ** block_scale(streams_of[3], (TOKENS, TOP), ((0, 128),), -0.2, 0.2), 0.1, 1.0)
    lengths = touch_ends(jax.random.randint(streams_of[4], (PROMPTS, K), 1, TOK_DEV + 1), jax.random.fold_in(streams_of[4], 1), 1, TOK_DEV).astype(jnp.int32)
    rewards = touch_ends(jax.random.randint(streams_of[5], (PROMPTS, K), -48, 49), jax.random.fold_in(streams_of[5], 1), -48, 48).astype(jnp.int32)
    w_gate = centred(streams_of[6], (EXPERTS, FF, D), D ** -0.5, 0.09375, ((0, 4), (1, 32)))
    w_up = centred(streams_of[7], (EXPERTS, FF, D), D ** -0.5, 0.09375, ((0, 4), (1, 32)))
    w_down = centred(streams_of[8], (EXPERTS, FF, D), FF ** -0.5, 0.0625, ((0, 4), (1, 32)))
    return dict(tokens=tokens, cotangent=cotangent, routes=routes, gate_weights=gate_weights, lengths=lengths, rewards=rewards, w_gate=w_gate, w_up=w_up, w_down=w_down)


def silu_parts(pre_gate):
    gate_prob = jax.nn.sigmoid(pre_gate)
    return pre_gate * gate_prob, gate_prob * (1.0 + pre_gate * (1.0 - gate_prob))


def reference(tokens, cotangent, routes, gate_weights, lengths, rewards, w_gate, w_up, w_down):
    devices = N_DP * N_EXPERT * N_SAMPLE
    slices = N_DP * N_SAMPLE
    width_slice = FF // slices
    choices_per = routes.shape[1]
    reward = rewards.astype(jnp.float32) * 0.0625
    reward_total = jnp.sum(reward, axis=1, keepdims=True)
    advantage = reward - (reward_total - reward) / (K - 1)
    owner = jnp.arange(TOKENS, dtype=jnp.int32) // TOK_DEV
    position = jnp.arange(TOKENS, dtype=jnp.int32) % TOK_DEV
    live = position < lengths.reshape(-1)[owner]
    weight_row = jnp.where(live, -advantage.reshape(-1)[owner], jnp.zeros((), jnp.float32))
    pair_scale = (gate_weights * weight_row[:, None]).reshape(-1)
    pair_expert = routes.reshape(-1)
    pair_count = pair_expert.shape[0]
    limit = devices * CAP
    member = (pair_expert[:, None] == jnp.arange(EXPERTS, dtype=jnp.int32)[None, :]).astype(jnp.int32)
    order = jnp.cumsum(member, axis=0) - 1
    where_row = jnp.where(member > 0, order, limit).astype(jnp.int32)
    pair_ids = jnp.broadcast_to(jnp.arange(pair_count, dtype=jnp.int32)[:, None], member.shape)
    expert_ids = jnp.broadcast_to(jnp.arange(EXPERTS, dtype=jnp.int32)[None, :], member.shape)
    table = jnp.zeros((EXPERTS, limit), jnp.int32).at[expert_ids, where_row].set(pair_ids, mode="drop")
    filled = jnp.arange(limit, dtype=jnp.int32)[None, :] < jnp.sum(member, axis=0)[:, None]

    def one_expert(packed):
        pair_rows, valid, gate_rows, up_rows, down_rows = packed
        token_rows = pair_rows // choices_per
        inputs = tokens[token_rows]
        scale = jnp.where(valid, pair_scale[pair_rows], jnp.zeros((), jnp.float32))
        grads_out = (cotangent[token_rows].astype(jnp.float32) * scale[:, None]).astype(jnp.bfloat16)
        pre_gate = jnp.dot(inputs, gate_rows.T, preferred_element_type=jnp.float32)
        pre_up = jnp.dot(inputs, up_rows.T, preferred_element_type=jnp.float32)
        active, derivative = silu_parts(pre_gate)
        hidden = (active * pre_up).astype(jnp.bfloat16)
        grad_hidden = jnp.dot(grads_out, down_rows.T, preferred_element_type=jnp.float32)
        grad_gate = (grad_hidden * pre_up * derivative).astype(jnp.bfloat16)
        grad_up = (grad_hidden * active).astype(jnp.bfloat16)
        down_grad = jnp.dot(hidden.T, grads_out, preferred_element_type=jnp.float32).astype(jnp.bfloat16)
        gate_grad = jnp.dot(grad_gate.T, inputs, preferred_element_type=jnp.float32).astype(jnp.bfloat16)
        up_grad = jnp.dot(grad_up.T, inputs, preferred_element_type=jnp.float32).astype(jnp.bfloat16)

        def add_slice(index, total):
            first = (index * width_slice).astype(jnp.int32)
            piece_gate = lax.dynamic_slice_in_dim(grad_gate, first, width_slice, 1)
            piece_up = lax.dynamic_slice_in_dim(grad_up, first, width_slice, 1)
            block_gate = lax.dynamic_slice_in_dim(gate_rows, first, width_slice, 0)
            block_up = lax.dynamic_slice_in_dim(up_rows, first, width_slice, 0)
            part = jnp.dot(piece_gate, block_gate, preferred_element_type=jnp.float32) + jnp.dot(piece_up, block_up, preferred_element_type=jnp.float32)
            rounded = lax.optimization_barrier(part.astype(jnp.bfloat16))
            return total + rounded.astype(jnp.float32)

        row_total = lax.fori_loop(0, slices, add_slice, jnp.zeros((limit, D), jnp.float32))
        return gate_grad, up_grad, down_grad, row_total.astype(jnp.bfloat16)

    grad_gate_all, grad_up_all, grad_down_all, row_grads = lax.map(one_expert, (table, filled, w_gate, w_up, w_down))
    token_rows = (table // choices_per).reshape(-1)
    masked = jnp.where(filled.reshape(-1)[:, None], row_grads.reshape(-1, D).astype(jnp.float32), jnp.zeros((), jnp.float32))
    grad_tokens = jnp.zeros((TOKENS, D), jnp.float32).at[token_rows].add(masked).astype(jnp.bfloat16)
    return grad_tokens, grad_gate_all, grad_up_all, grad_down_all
```

```python
import functools

import jax
import jax.numpy as jnp
from jax import lax
from jax.experimental import pallas as pl
from jax.experimental.pallas import tpu as pltpu
from jax.sharding import PartitionSpec as P

CAP = 6
RING = 4
WIDTH = 4096
META = 128
ROWS = 40
MESH = pl.DeviceIdType.MESH
ORDERS = (("x", "y", "z"), ("y", "z", "x"), ("z", "x", "y"))
BF = jnp.bfloat16
F32 = jnp.float32


def place():
    dp = lax.axis_index("dp")
    ex = lax.axis_index("expert")
    return {"x": lax.axis_index("sample"), "y": (dp % 2) * 2 + ex // 2, "z": dp // 2}, ex % 2


def device(at, core):
    return {
        "dp": at["z"] * 2 + at["y"] // 2,
        "expert": (at["y"] % 2) * 2 + core,
        "sample": at["x"],
    }


def moved(at, axis, by):
    return {**at, axis: lax.rem(at[axis] + (by + RING), RING)}


def greet(at, core):
    barrier = pltpu.get_barrier_semaphore()
    peers = [device(moved(at, axis, by), core) for axis in "xyz" for by in (1, -1)]
    peers.append(device(at, 1 - core))
    for peer in peers:
        pl.semaphore_signal(barrier, inc=1, device_id=peer, device_id_type=MESH)
    pl.semaphore_wait(barrier, len(peers))


def remote(src, dst, send, recv, peer):
    return pltpu.make_async_remote_copy(
        src_ref=src, dst_ref=dst, send_sem=send, recv_sem=recv, device_id=peer, device_id_type=MESH
    )


GATHER_COPIES = 35


def gather_kernel(own_ref, out_ref, mate, block, send, recv, keep):
    at, core = place()
    partner = device(at, 1 - core)
    greet(at, core)
    swap = remote(own_ref.at[1 - core], mate, send.at[3, 0], recv.at[3, 0], partner)
    swap.start()
    swap.wait()

    @pl.when(core == 0)
    def _():
        block[0:20] = own_ref[0]
        block[20:40] = mate[...]

    @pl.when(core == 1)
    def _():
        block[0:20] = mate[...]
        block[20:40] = own_ref[1]

    here = pltpu.make_async_copy(block, out_ref.at[core, at["z"], at["y"], at["x"]], keep)
    here.start()
    part = (WIDTH + META) // 3
    copies = {}

    def view(p, **over):
        to = {**at, **over}
        return out_ref.at[core, to["z"], to["y"], to["x"], :, pl.ds(p * part, part)]

    def push(p, k, src, dst, peer):
        copy = remote(src, dst, send.at[p, k], recv.at[p, k], peer)
        copy.start()
        copies[p, k] = copy

    def hand(p, k, ref):
        push(p, k, ref, ref, partner)

    def near(axis, by):
        return device(moved(at, axis, by), core)

    def coord(axis, by):
        return at[axis] if by == 0 else moved(at, axis, by)[axis]

    every = pl.ds(0, RING)
    offset = (0, -1, 1, 2)

    def line(p, l, plane=0):
        d1, d2, d3 = ORDERS[p]
        return view(p, **{d1: every, d2: coord(d2, offset[l]), d3: coord(d3, plane)})

    def spread(p, l):
        d3 = ORDERS[p][2]
        for k, by in enumerate((1, -1)):
            push(p, 7 + 2 * l + k, line(p, l), line(p, l), near(d3, by))
        hand(p, 19 + l, line(p, l))

    for p, (d1, d2, d3) in enumerate(ORDERS):
        mine = block.at[:, pl.ds(p * part, part)]
        push(p, 0, mine, view(p), near(d1, 1))
        push(p, 1, mine, view(p), near(d1, -1))
    for p, (d1, d2, d3) in enumerate(ORDERS):
        copies[p, 0].wait_recv()
        got = view(p, **{d1: coord(d1, -1)})
        push(p, 2, got, got, near(d1, 1))
    here.wait()
    for p, (d1, d2, d3) in enumerate(ORDERS):
        copies[p, 1].wait_recv()
        copies[p, 2].wait_recv()
        push(p, 3, line(p, 0), line(p, 0), near(d2, 1))
        push(p, 4, line(p, 0), line(p, 0), near(d2, -1))
    for p in range(3):
        spread(p, 0)
    for p, (d1, d2, d3) in enumerate(ORDERS):
        copies[p, 3].wait_recv()
        got = view(p, **{d1: pl.ds(0, 2), d2: coord(d2, -1)})
        push(p, 5, got, got, near(d2, 1))
        copies[p, 4].wait_recv()
        got = view(p, **{d1: pl.ds(2, 2), d2: coord(d2, 1)})
        push(p, 6, got, got, near(d2, -1))
    for p in range(3):
        spread(p, 1)
        spread(p, 2)

    def arrived(p, l):
        d3 = ORDERS[p][2]
        for k, by in enumerate((1, -1)):
            copies[p, 7 + 2 * l + k].wait_recv()
            got = line(p, l, -by)
            if k == l // 2:
                push(p, 15 + l, got, got, near(d3, by))
            hand(p, 23 + 4 * k + l, got)

    for p in range(3):
        arrived(p, 0)
    for p in range(3):
        copies[p, 5].wait_recv()
        copies[p, 6].wait_recv()
        spread(p, 3)
    for l in (1, 2, 3):
        for p in range(3):
            arrived(p, l)
    for l in range(4):
        for p in range(3):
            copies[p, 15 + l].wait_recv()
            hand(p, 31 + l, line(p, l, 2))
    for p in range(3):
        for k in range(19, GATHER_COPIES):
            copies[p, k].wait_recv()
    for copy in copies.values():
        copy.wait_send()


def gather_rows(own):
    return pl.pallas_call(
        gather_kernel,
        out_shape=jax.ShapeDtypeStruct((2, RING, RING, RING, ROWS, WIDTH + META), BF),
        in_specs=[pl.BlockSpec(memory_space=pltpu.VMEM)],
        out_specs=pl.BlockSpec(memory_space=pl.ANY),
        scratch_shapes=[
            pltpu.VMEM((ROWS // 2, WIDTH + META), BF),
            pltpu.VMEM((ROWS, WIDTH + META), BF),
            pltpu.SemaphoreType.DMA((4, GATHER_COPIES)),
            pltpu.SemaphoreType.DMA((4, GATHER_COPIES)),
            pltpu.SemaphoreType.DMA,
        ],
        compiler_params=pltpu.CompilerParams(collective_id=0, has_side_effects=True),
        name="gather_rows",
    )(own)


HALF = WIDTH // 2
WIDTHS = (768, 640, 640)
STARTS = (0, 768, 1408)
AHEAD = (3, 1)
BEHIND = (2, 0)


def scatter_kernel(p_ref, out_ref, *scratch):
    acc, mate, fa, ma, pa, fb, mb, pb, fc, mc, pc = [scratch[3 * i : 3 * i + 3] for i in range(11)]
    done, other_done, load, load_far, far_in, send, recv = scratch[33:]
    at, core = place()
    partner = device(at, 1 - core)
    greet(at, core)
    copies = {}
    every = pl.ds(0, RING)
    offset = (0, -1, 1, 2)

    def near(axis, by):
        return device(moved(at, axis, by), core)

    def coord(axis, by):
        return at[axis] if by == 0 else moved(at, axis, by)[axis]

    def spot(**over):
        to = {**at, **over}
        return to["z"], to["y"], to["x"]

    def plane_at(p, by):
        d1, d2, d3 = ORDERS[p]
        return spot(**{d1: every, d2: every, d3: coord(d3, by)})

    def columns(p, side):
        return pl.ds(pl.multiple_of(side * HALF + STARTS[p], 128), WIDTHS[p])

    def push(p, key, k, src, dst, peer):
        copy = remote(src, dst, send.at[p, k], recv.at[p, k], peer)
        copy.start()
        copies[(p,) + key] = copy

    loads = {}
    for n, by in enumerate((2, 1, -1, 0)):
        for p in range(3):
            where = plane_at(p, by)
            far = remote(
                p_ref.at[where + (slice(None), columns(p, 1 - core))],
                mate[p].at[where],
                load_far.at[p, n],
                far_in.at[p, n],
                partner,
            )
            far.start()
            own = pltpu.make_async_copy(
                p_ref.at[where + (slice(None), columns(p, core))], acc[p].at[where], load.at[p, n]
            )
            own.start()
            loads[p, by] = (own, far)

    def add(dst, index, *terms):
        total = dst[index].astype(F32)
        for ref, where in terms:
            total = total + ref[where].astype(F32)
        dst[index] = total.astype(BF)

    def ready(p, by):
        own, far = loads[p, by]
        own.wait()
        far.wait_recv()
        d1, d2, d3 = ORDERS[p]

        def body(i, carry):
            where = spot(**{d1: i % RING, d2: i // RING, d3: coord(d3, by)})
            add(acc[p], where, (mate[p], where))
            return carry

        lax.fori_loop(0, RING * RING, body, 0)

    def line(p, r, by):
        d1, d2, d3 = ORDERS[p]
        return acc[p].at[spot(**{d1: every, d2: coord(d2, offset[r]), d3: coord(d3, by)})]

    def add_line(p, r, by, *terms, first=0, count=RING):
        d1, d2, d3 = ORDERS[p]

        def body(i, carry):
            where = spot(**{d1: i, d2: coord(d2, offset[r]), d3: coord(d3, by)})
            add(acc[p], where, *[(ref, (r, i) if lead else (i,)) for ref, lead in terms])
            return carry

        lax.fori_loop(first, first + count, body, 0)

    for p in range(3):
        ready(p, 2)
        for r in (3, 2, 1, 0):
            push(p, ("fa", r), r, line(p, r, 2), fa[p].at[r], near(ORDERS[p][2], 1 if r in AHEAD else -1))
    for p in range(3):
        ready(p, 1)
        for r in BEHIND:
            push(p, ("ma", r), 4 + r, line(p, r, 1), ma[p].at[r], near(ORDERS[p][2], 1))
    for p in range(3):
        ready(p, -1)
        for r in AHEAD:
            push(p, ("pa", r), 8 + r, line(p, r, -1), pa[p].at[r], near(ORDERS[p][2], -1))
    for p in range(3):
        ready(p, 0)
    for r in (3, 2, 1, 0):
        for p in range(3):
            copies[p, "fa", r].wait_recv()
            if r in AHEAD:
                add_line(p, r, 1, (fa[p], True))
                push(p, ("ma", r), 4 + r, line(p, r, 1), ma[p].at[r], near(ORDERS[p][2], 1))
            else:
                add_line(p, r, -1, (fa[p], True))
                push(p, ("pa", r), 8 + r, line(p, r, -1), pa[p].at[r], near(ORDERS[p][2], -1))

    def piece(p, r, half):
        d1, d2, d3 = ORDERS[p]
        return acc[p].at[spot(**{d1: pl.ds(2 * half, 2), d2: coord(d2, offset[r])})]

    def half_of(ref, half):
        return ref.at[pl.ds(2 * half, 2)]

    for r in (3, 2, 1, 0):
        for p in range(3):
            copies[p, "ma", r].wait_recv()
            copies[p, "pa", r].wait_recv()
            add_line(p, r, 0, (ma[p], True), (pa[p], True))
            d2 = ORDERS[p][1]
            if r == 3:
                push(p, ("fb", 0), 12, piece(p, 3, 0), half_of(fb[p], 0), near(d2, 1))
                push(p, ("fb", 1), 13, piece(p, 3, 1), half_of(fb[p], 1), near(d2, -1))
            if r == 2:
                push(p, ("mb", 1), 15, piece(p, 2, 1), half_of(mb[p], 1), near(d2, 1))
            if r == 1:
                push(p, ("pb", 0), 16, piece(p, 1, 0), half_of(pb[p], 0), near(d2, -1))
    for p in range(3):
        d2 = ORDERS[p][1]
        copies[p, "fb", 0].wait_recv()
        add_line(p, 2, 0, (fb[p], False), first=0, count=2)
        push(p, ("mb", 0), 14, piece(p, 2, 0), half_of(mb[p], 0), near(d2, 1))
        copies[p, "fb", 1].wait_recv()
        add_line(p, 1, 0, (fb[p], False), first=2, count=2)
        push(p, ("pb", 1), 17, piece(p, 1, 1), half_of(pb[p], 1), near(d2, -1))

    def cell(p, by):
        d1 = ORDERS[p][0]
        return spot(**{d1: coord(d1, by)})

    for p in range(3):
        d1 = ORDERS[p][0]
        for half in (0, 1):
            copies[p, "mb", half].wait_recv()
            copies[p, "pb", half].wait_recv()
        add_line(p, 0, 0, (mb[p], False), (pb[p], False))
        push(p, ("fc",), 18, acc[p].at[cell(p, 2)], fc[p], near(d1, 1))
        push(p, ("pc",), 20, acc[p].at[cell(p, -1)], pc[p], near(d1, -1))
    for p in range(3):
        d1 = ORDERS[p][0]
        copies[p, "fc"].wait_recv()
        add(acc[p], cell(p, 1), (fc[p], ...))
        push(p, ("mc",), 19, acc[p].at[cell(p, 1)], mc[p], near(d1, 1))
    for p in range(3):
        copies[p, "pc"].wait_recv()
        copies[p, "mc"].wait_recv()
        own = acc[p][cell(p, 0)].astype(F32) + pc[p][...].astype(F32) + mc[p][...].astype(F32)
        done[:, STARTS[p] : STARTS[p] + WIDTHS[p]] = own.astype(BF)
    last = remote(done, other_done, send.at[3, 0], recv.at[3, 0], partner)
    last.start()
    last.wait_recv()

    @pl.when(core == 0)
    def _():
        out_ref[:, :HALF] = done[0:20]
        out_ref[:, HALF:] = other_done[0:20]

    @pl.when(core == 1)
    def _():
        out_ref[:, :HALF] = other_done[20:40]
        out_ref[:, HALF:] = done[20:40]

    last.wait_send()
    for copy in copies.values():
        copy.wait_send()
    for _, far in loads.values():
        far.wait_send()


def scatter_sum(partial):
    full = [pltpu.VMEM((RING, RING, RING, ROWS, w), BF) for w in WIDTHS]
    lines = [pltpu.VMEM((RING, RING, ROWS, w), BF) for w in WIDTHS]
    line = [pltpu.VMEM((RING, ROWS, w), BF) for w in WIDTHS]
    cell = [pltpu.VMEM((ROWS, w), BF) for w in WIDTHS]
    return pl.pallas_call(
        scatter_kernel,
        out_shape=jax.ShapeDtypeStruct((ROWS // 2, WIDTH), BF),
        in_specs=[pl.BlockSpec(memory_space=pl.ANY)],
        out_specs=pl.BlockSpec(memory_space=pltpu.VMEM),
        scratch_shapes=full * 2
        + lines * 3
        + line * 3
        + cell * 3
        + [pltpu.VMEM((ROWS, HALF), BF)] * 2
        + [pltpu.SemaphoreType.DMA((3, 4))] * 3
        + [pltpu.SemaphoreType.DMA((4, 21))] * 2,
        compiler_params=pltpu.CompilerParams(
            collective_id=1, has_side_effects=True, vmem_limit_bytes=60 * 1024 * 1024
        ),
        name="scatter_sum",
    )(partial)


GROUP = 160
SLOTS = 48


def turned(a, b):
    return lax.dot_general(a, b, (((0,), (0,)), ((), ())), preferred_element_type=F32)


def select_kernel(group_ref, all_ref, x_ref, g_ref, pick_ref):
    info = all_ref[0, 0, :, WIDTH:]
    meta = info.astype(F32)
    row = lax.broadcasted_iota(jnp.int32, (GROUP, 1), 0)
    lane = lax.broadcasted_iota(jnp.int32, (GROUP, 128), 1)
    same = lax.broadcasted_iota(jnp.int32, (GROUP, GROUP), 0) % ROWS == (
        lax.broadcasted_iota(jnp.int32, (GROUP, GROUP), 1) % ROWS
    )
    total = jnp.dot(same.astype(F32).astype(BF), info, preferred_element_type=F32)[:, 9:10] * 0.0625
    reward = meta[:, 9:10] * 0.0625
    advantage = reward - (total - reward) / 3.0
    live = (row % 20).astype(F32) < meta[:, 8:9]
    weight = jnp.where(live, -advantage, 0.0)
    first = (2 * group_ref[0]).astype(F32)
    scale = jnp.zeros((128, 128), F32)
    pick = jnp.zeros((GROUP, 128), F32)
    for k in range(2):
        j = meta[:, k : k + 1] - first
        valid = (j >= 0.0) & (j < 2.0)
        slot = j * SLOTS + ((row // 20) * CAP).astype(F32) + meta[:, 10 + k : 11 + k]
        slot = jnp.where(valid, slot, -1.0).astype(jnp.int32)
        one = (lane == slot).astype(F32)
        pick = pick + one
        c = 2 + 3 * k
        value = ((meta[:, c : c + 1] + meta[:, c + 1 : c + 2]) + meta[:, c + 2 : c + 3]) * weight
        high = value.astype(BF).astype(F32)
        middle = (value - high).astype(BF).astype(F32)
        low = value - high - middle
        pieces = jnp.where(lane == 0, high, jnp.where(lane == 1, middle, jnp.where(lane == 2, low, 0.0)))
        scale = scale + turned(one.astype(BF), pieces.astype(BF))
    column = (scale[:, 0:1] + scale[:, 1:2]) + scale[:, 2:3]
    pick = pick.astype(BF)
    pick_ref[0] = pick
    for start in range(0, WIDTH, 1024):
        cols = slice(start, start + 1024)
        x = turned(pick, all_ref[0, 0, :, cols]).astype(BF)
        g = (turned(pick, all_ref[1, 0, :, cols]) * column).astype(BF)
        for j in range(2):
            x_ref[j, :, cols] = x[j * SLOTS : (j + 1) * SLOTS]
            g_ref[j, :, cols] = g[j * SLOTS : (j + 1) * SLOTS]


def select_rows(group, everything):
    blocks = everything.shape[1]
    rows = jax.ShapeDtypeStruct((2, blocks * SLOTS, WIDTH), BF)
    return pl.pallas_call(
        select_kernel,
        grid=(blocks,),
        out_shape=(rows, rows, jax.ShapeDtypeStruct((blocks, GROUP, 128), BF)),
        in_specs=[
            pl.BlockSpec(memory_space=pltpu.SMEM),
            pl.BlockSpec((2, 1, GROUP, WIDTH + META), lambda b: (0, b, 0, 0)),
        ],
        out_specs=(
            pl.BlockSpec((2, SLOTS, WIDTH), lambda b: (0, b, 0)),
            pl.BlockSpec((2, SLOTS, WIDTH), lambda b: (0, b, 0)),
            pl.BlockSpec((1, GROUP, 128), lambda b: (b, 0, 0)),
        ),
        name="select_rows",
    )(group, everything)


def combine_kernel(pick_ref, r_ref, out_ref):
    for start in range(0, WIDTH, 1024):
        cols = slice(start, start + 1024)
        total = jnp.dot(pick_ref[0, :, :SLOTS], r_ref[0, :, cols], preferred_element_type=F32)
        total += jnp.dot(pick_ref[0, :, SLOTS : 2 * SLOTS], r_ref[1, :, cols], preferred_element_type=F32)
        out_ref[0, :, cols] = total.astype(BF)


def combine_rows(pick, rows):
    blocks = pick.shape[0]
    return pl.pallas_call(
        combine_kernel,
        grid=(blocks,),
        out_shape=jax.ShapeDtypeStruct((blocks, GROUP, WIDTH), BF),
        in_specs=[
            pl.BlockSpec((1, GROUP, 128), lambda b: (b, 0, 0)),
            pl.BlockSpec((2, SLOTS, WIDTH), lambda b: (0, b, 0)),
        ],
        out_specs=pl.BlockSpec((1, GROUP, WIDTH), lambda b: (b, 0, 0)),
        name="combine_rows",
    )(pick, rows)


def three(values):
    high = lax.reduce_precision(values, 8, 7)
    middle = lax.reduce_precision(values - high, 8, 7)
    return [high, middle, values - high - middle]


def own_rows(tokens, cotangent, routes, gate_weights, lengths, rewards):
    count = tokens.shape[0]
    flat = routes.reshape(-1)
    before = jnp.arange(2 * count)[:, None] > jnp.arange(2 * count)[None, :]
    same = flat[:, None] == flat[None, :]
    earlier = jnp.sum((before & same).astype(jnp.int32), axis=1).reshape(count, 2)
    wide = jnp.ones((count, 1), F32)
    columns = [routes.astype(F32)]
    for k in range(2):
        columns += three(gate_weights[:, k : k + 1])
    columns += [wide * lengths[0, 0].astype(F32), wide * rewards[0, 0].astype(F32), earlier.astype(F32)]
    meta = jnp.concatenate(columns, axis=1)
    meta = jnp.pad(meta, ((0, 0), (0, META - meta.shape[1]))).astype(BF)
    return jnp.stack(
        [jnp.concatenate([tokens, meta], axis=1), jnp.concatenate([cotangent, jnp.zeros_like(meta)], axis=1)]
    )


def local(tokens, cotangent, routes, gate_weights, lengths, rewards, w_gate, w_up, w_down):
    own = own_rows(tokens, cotangent, routes, gate_weights, lengths, rewards)
    everything = gather_rows(own)
    everything = everything.reshape(2, RING * RING, GROUP, WIDTH + META)
    group = lax.axis_index("expert").astype(jnp.int32).reshape(1)
    x, g, pick = select_rows(group, everything)
    forward = functools.partial(jnp.einsum, "jcd,jfd->jcf", preferred_element_type=F32)
    back = functools.partial(jnp.einsum, "jcf,jfd->jcd", preferred_element_type=F32)
    weigh = functools.partial(jnp.einsum, "jcf,jcd->jfd", preferred_element_type=F32)
    pre_gate, pre_up, grad_hidden = forward(x, w_gate), forward(x, w_up), forward(g, w_down)
    prob = jax.nn.sigmoid(pre_gate)
    active = pre_gate * prob
    hidden = (active * pre_up).astype(BF)
    grad_gate = (grad_hidden * pre_up * (prob * (1.0 + pre_gate * (1.0 - prob)))).astype(BF)
    grad_up = (grad_hidden * active).astype(BF)
    rows = (back(grad_gate, w_gate) + back(grad_up, w_up)).astype(BF)
    partial = combine_rows(pick, rows).reshape(RING, RING, RING, ROWS, WIDTH)
    grad_tokens = scatter_sum(partial)
    return (
        grad_tokens,
        weigh(grad_gate, x).astype(BF),
        weigh(grad_up, x).astype(BF),
        weigh(hidden, g).astype(BF),
    )


def solution(mesh):
    rows = P(("dp", "expert", "sample"), None)
    pair = P(("dp", "expert"), "sample")
    weights = P("expert", ("dp", "sample"), None)
    return jax.shard_map(
        local,
        mesh=mesh,
        in_specs=(rows,) * 4 + (pair,) * 2 + (weights,) * 3,
        out_specs=(rows,) + (weights,) * 3,
        check_vma=False,
    )
```

```python
import functools

import jax
import jax.numpy as jnp
from jax import lax
from jax.experimental import pallas as pl
from jax.experimental.pallas import tpu as pltpu
from jax.sharding import PartitionSpec as P

CAP = 6
RING = 4
WIDTH = 4096
META = 128
ROWS = 40
MESH = pl.DeviceIdType.MESH
ORDERS = (("x", "y", "z"), ("y", "z", "x"), ("z", "x", "y"))
BF = jnp.bfloat16
F32 = jnp.float32


def place():
    dp = lax.axis_index("dp")
    ex = lax.axis_index("expert")
    return {"x": lax.axis_index("sample"), "y": (dp % 2) * 2 + ex // 2, "z": dp // 2}, ex % 2


def device(at, core):
    return {
        "dp": at["z"] * 2 + at["y"] // 2,
        "expert": (at["y"] % 2) * 2 + core,
        "sample": at["x"],
    }


def moved(at, axis, by):
    return {**at, axis: lax.rem(at[axis] + (by + RING), RING)}


def greet(at, core):
    barrier = pltpu.get_barrier_semaphore()
    peers = [device(moved(at, axis, by), core) for axis in "xyz" for by in (1, -1)]
    peers.append(device(at, 1 - core))
    for peer in peers:
        pl.semaphore_signal(barrier, inc=1, device_id=peer, device_id_type=MESH)
    pl.semaphore_wait(barrier, len(peers))


def remote(src, dst, send, recv, peer):
    return pltpu.make_async_remote_copy(
        src_ref=src, dst_ref=dst, send_sem=send, recv_sem=recv, device_id=peer, device_id_type=MESH
    )


GATHER_COPIES = 35


def gather_kernel(own_ref, out_ref, mate, block, send, recv, keep):
    at, core = place()
    partner = device(at, 1 - core)
    greet(at, core)
    swap = remote(own_ref.at[1 - core], mate, send.at[3, 0], recv.at[3, 0], partner)
    swap.start()
    swap.wait()

    @pl.when(core == 0)
    def _():
        block[0:20] = own_ref[0]
        block[20:40] = mate[...]

    @pl.when(core == 1)
    def _():
        block[0:20] = mate[...]
        block[20:40] = own_ref[1]

    here = pltpu.make_async_copy(block, out_ref.at[core, at["z"], at["y"], at["x"]], keep)
    here.start()
    part = (WIDTH + META) // 3
    copies = {}

    def view(p, **over):
        to = {**at, **over}
        return out_ref.at[core, to["z"], to["y"], to["x"], :, pl.ds(p * part, part)]

    def push(p, k, src, dst, peer):
        copy = remote(src, dst, send.at[p, k], recv.at[p, k], peer)
        copy.start()
        copies[p, k] = copy

    def hand(p, k, ref):
        push(p, k, ref, ref, partner)

    def near(axis, by):
        return device(moved(at, axis, by), core)

    def coord(axis, by):
        return at[axis] if by == 0 else moved(at, axis, by)[axis]

    every = pl.ds(0, RING)
    offset = (0, -1, 1, 2)

    def line(p, l, plane=0):
        d1, d2, d3 = ORDERS[p]
        return view(p, **{d1: every, d2: coord(d2, offset[l]), d3: coord(d3, plane)})

    def spread(p, l):
        d3 = ORDERS[p][2]
        for k, by in enumerate((1, -1)):
            push(p, 7 + 2 * l + k, line(p, l), line(p, l), near(d3, by))
        hand(p, 19 + l, line(p, l))

    for p, (d1, d2, d3) in enumerate(ORDERS):
        mine = block.at[:, pl.ds(p * part, part)]
        push(p, 0, mine, view(p), near(d1, 1))
        push(p, 1, mine, view(p), near(d1, -1))
    for p, (d1, d2, d3) in enumerate(ORDERS):
        copies[p, 0].wait_recv()
        got = view(p, **{d1: coord(d1, -1)})
        push(p, 2, got, got, near(d1, 1))
    here.wait()
    for p, (d1, d2, d3) in enumerate(ORDERS):
        copies[p, 1].wait_recv()
        copies[p, 2].wait_recv()
        push(p, 3, line(p, 0), line(p, 0), near(d2, 1))
        push(p, 4, line(p, 0), line(p, 0), near(d2, -1))
    for p in range(3):
        spread(p, 0)
    for p, (d1, d2, d3) in enumerate(ORDERS):
        copies[p, 3].wait_recv()
        got = view(p, **{d1: pl.ds(0, 2), d2: coord(d2, -1)})
        push(p, 5, got, got, near(d2, 1))
        copies[p, 4].wait_recv()
        got = view(p, **{d1: pl.ds(2, 2), d2: coord(d2, 1)})
        push(p, 6, got, got, near(d2, -1))
    for p in range(3):
        spread(p, 1)
        spread(p, 2)

    def arrived(p, l):
        d3 = ORDERS[p][2]
        for k, by in enumerate((1, -1)):
            copies[p, 7 + 2 * l + k].wait_recv()
            got = line(p, l, -by)
            if k == l // 2:
                push(p, 15 + l, got, got, near(d3, by))
            hand(p, 23 + 4 * k + l, got)

    for p in range(3):
        arrived(p, 0)
    for p in range(3):
        copies[p, 5].wait_recv()
        copies[p, 6].wait_recv()
        spread(p, 3)
    for l in (1, 2, 3):
        for p in range(3):
            arrived(p, l)
    for l in range(4):
        for p in range(3):
            copies[p, 15 + l].wait_recv()
            hand(p, 31 + l, line(p, l, 2))
    for p in range(3):
        for k in range(19, GATHER_COPIES):
            copies[p, k].wait_recv()
    for copy in copies.values():
        copy.wait_send()


def gather_rows(own):
    return pl.pallas_call(
        gather_kernel,
        out_shape=jax.ShapeDtypeStruct((2, RING, RING, RING, ROWS, WIDTH + META), BF),
        in_specs=[pl.BlockSpec(memory_space=pltpu.VMEM)],
        out_specs=pl.BlockSpec(memory_space=pl.ANY),
        scratch_shapes=[
            pltpu.VMEM((ROWS // 2, WIDTH + META), BF),
            pltpu.VMEM((ROWS, WIDTH + META), BF),
            pltpu.SemaphoreType.DMA((4, GATHER_COPIES)),
            pltpu.SemaphoreType.DMA((4, GATHER_COPIES)),
            pltpu.SemaphoreType.DMA,
        ],
        compiler_params=pltpu.CompilerParams(collective_id=0, has_side_effects=True),
        name="gather_rows",
    )(own)


GROUP = 160
SLOTS = 48

HALF = WIDTH // 2
WIDTHS = (384, 384, 256, 384, 256, 384)
STARTS = (0, 384, 768, 1024, 1408, 1664)
WIDEST = 384
STREAMS = 6
STREAM_COPIES = 22
AHEAD = (3, 1)
BEHIND = (2, 0)


def finish_kernel(gg_ref, gu_ref, pick_ref, wg_ref, wu_ref, out_ref, *scratch):
    n = STREAMS
    acc, mate, fa, ma, pa, fb, mb, pb, fc, mc, pc = [scratch[n * i : n * i + n] for i in range(11)]
    give, weights, rows, done, other_done, wsem, send, recv = scratch[11 * n :]
    at, core = place()
    partner = device(at, 1 - core)
    copies = {}
    every = pl.ds(0, RING)
    offset = (0, -1, 1, 2)

    def near(axis, by):
        return device(moved(at, axis, by), core)

    def coord(axis, by):
        return at[axis] if by == 0 else moved(at, axis, by)[axis]

    def spot(**over):
        to = {**at, **over}
        return to["z"], to["y"], to["x"]

    def order(s):
        return ORDERS[s % 3]

    def push(s, key, k, src, dst, peer):
        copy = remote(src, dst, send.at[s, k], recv.at[s, k], peer)
        copy.start()
        copies[(s,) + key] = copy

    turns = [(s, far) for c in (0, 3) for far in (True, False) for s in range(c, c + 3)]

    def fetch(turn):
        s, far = turns[turn]
        side = 1 - core if far else core
        columns = pl.ds(pl.multiple_of(side * HALF + STARTS[s], 128), WIDTHS[s])
        got = []
        for k, ref in enumerate((wg_ref, wu_ref)):
            to = weights.at[turn % 2, k, :, :, pl.ds(0, WIDTHS[s])]
            got.append(pltpu.make_async_copy(ref.at[:, :, columns], to, wsem.at[turn % 2, k]))
            got[-1].start()
        return got

    fetched = {0: fetch(0)}

    def compute(turn):
        s, far = turns[turn]
        w = WIDTHS[s]
        slot = turn % 2
        if turn + 1 < len(turns):
            fetched[turn + 1] = fetch(turn + 1)
        for copy in fetched[turn]:
            copy.wait()
        part = 8 * SLOTS

        def product(i, carry):
            j, half = i // 2, i % 2
            take = pl.ds(pl.multiple_of(half * part, part), part)
            total = jnp.dot(gg_ref[j, take, :], weights[slot, 0, j, :, :w], preferred_element_type=F32)
            total += jnp.dot(gu_ref[j, take, :], weights[slot, 1, j, :, :w], preferred_element_type=F32)
            total = total.astype(BF)
            for l in range(8):
                rows[half * 8 + l, j, :, :w] = total[l * SLOTS : (l + 1) * SLOTS]
            return carry

        lax.fori_loop(0, 4, product, 0)
        if far:
            if s >= 3:
                copies[s - 3, "far"].wait_send()
        else:
            copies[s, "far"].wait_recv()

        def place_rows(l, carry):
            z, y = l // RING, l % RING
            total = jnp.dot(
                pick_ref[l, :, : 2 * SLOTS], rows[l, :, :, :w].reshape(2 * SLOTS, w), preferred_element_type=F32
            )
            for x in range(RING):
                piece = total[x * ROWS : (x + 1) * ROWS]
                if far:
                    give[s % 3, z, y, x, :, :w] = piece.astype(BF)
                else:
                    acc[s][z, y, x] = (piece + mate[s][z, y, x].astype(F32)).astype(BF)
            return carry

        lax.fori_loop(0, RING * RING, place_rows, 0)
        if far:
            push(s, ("far",), 21, give.at[s % 3, :, :, :, :, pl.ds(0, w)], mate[s], partner)

    def add(dst, index, *terms):
        total = dst[index].astype(F32)
        for ref, where in terms:
            total = total + ref[where].astype(F32)
        dst[index] = total.astype(BF)

    def line(s, r, by):
        d1, d2, d3 = order(s)
        return acc[s].at[spot(**{d1: every, d2: coord(d2, offset[r]), d3: coord(d3, by)})]

    def add_line(s, r, by, *terms, first=0, count=RING):
        d1, d2, d3 = order(s)

        def body(i, carry):
            where = spot(**{d1: i, d2: coord(d2, offset[r]), d3: coord(d3, by)})
            add(acc[s], where, *[(ref, (r, i) if lead else (i,)) for ref, lead in terms])
            return carry

        lax.fori_loop(first, first + count, body, 0)

    def piece(s, r, half):
        d1, d2, d3 = order(s)
        return acc[s].at[spot(**{d1: pl.ds(2 * half, 2), d2: coord(d2, offset[r])})]

    def half_of(ref, half):
        return ref.at[pl.ds(2 * half, 2)]

    def cell(s, by):
        d1 = order(s)[0]
        return spot(**{d1: coord(d1, by)})

    def travel(streams):
        for s in streams:
            d3 = order(s)[2]
            for r in (3, 2, 1, 0):
                push(s, ("fa", r), r, line(s, r, 2), fa[s].at[r], near(d3, 1 if r in AHEAD else -1))
            for r in BEHIND:
                push(s, ("ma", r), 4 + r, line(s, r, 1), ma[s].at[r], near(d3, 1))
            for r in AHEAD:
                push(s, ("pa", r), 8 + r, line(s, r, -1), pa[s].at[r], near(d3, -1))
        yield
        for r in (3, 2, 1, 0):
            for s in streams:
                d3 = order(s)[2]
                copies[s, "fa", r].wait_recv()
                if r in AHEAD:
                    add_line(s, r, 1, (fa[s], True))
                    push(s, ("ma", r), 4 + r, line(s, r, 1), ma[s].at[r], near(d3, 1))
                else:
                    add_line(s, r, -1, (fa[s], True))
                    push(s, ("pa", r), 8 + r, line(s, r, -1), pa[s].at[r], near(d3, -1))
                yield
        for r in (3, 2, 1, 0):
            for s in streams:
                d2 = order(s)[1]
                copies[s, "ma", r].wait_recv()
                copies[s, "pa", r].wait_recv()
                add_line(s, r, 0, (ma[s], True), (pa[s], True))
                if r == 3:
                    push(s, ("fb", 0), 12, piece(s, 3, 0), half_of(fb[s], 0), near(d2, 1))
                    push(s, ("fb", 1), 13, piece(s, 3, 1), half_of(fb[s], 1), near(d2, -1))
                if r == 2:
                    push(s, ("mb", 1), 15, piece(s, 2, 1), half_of(mb[s], 1), near(d2, 1))
                if r == 1:
                    push(s, ("pb", 0), 16, piece(s, 1, 0), half_of(pb[s], 0), near(d2, -1))
                yield
        for s in streams:
            d2 = order(s)[1]
            copies[s, "fb", 0].wait_recv()
            add_line(s, 2, 0, (fb[s], False), first=0, count=2)
            push(s, ("mb", 0), 14, piece(s, 2, 0), half_of(mb[s], 0), near(d2, 1))
            copies[s, "fb", 1].wait_recv()
            add_line(s, 1, 0, (fb[s], False), first=2, count=2)
            push(s, ("pb", 1), 17, piece(s, 1, 1), half_of(pb[s], 1), near(d2, -1))
            yield
        for s in streams:
            d1 = order(s)[0]
            for half in (0, 1):
                copies[s, "mb", half].wait_recv()
                copies[s, "pb", half].wait_recv()
            add_line(s, 0, 0, (mb[s], False), (pb[s], False))
            push(s, ("fc",), 18, acc[s].at[cell(s, 2)], fc[s], near(d1, 1))
            push(s, ("pc",), 20, acc[s].at[cell(s, -1)], pc[s], near(d1, -1))
            yield
        for s in streams:
            d1 = order(s)[0]
            copies[s, "fc"].wait_recv()
            add(acc[s], cell(s, 1), (fc[s], ...))
            push(s, ("mc",), 19, acc[s].at[cell(s, 1)], mc[s], near(d1, 1))
            yield
        for s in streams:
            copies[s, "pc"].wait_recv()
            copies[s, "mc"].wait_recv()
            own = acc[s][cell(s, 0)].astype(F32) + pc[s][...].astype(F32) + mc[s][...].astype(F32)
            done[:, STARTS[s] : STARTS[s] + WIDTHS[s]] = own.astype(BF)
            yield

    def forward(journey, count):
        for _ in range(count):
            next(journey, None)

    greet(at, core)
    for turn in range(6):
        compute(turn)
    early = travel((0, 1, 2))
    forward(early, 1)
    for turn in (6, 7, 8):
        compute(turn)
    forward(early, 3)
    for turn in (9, 10):
        compute(turn)
    forward(early, 3)
    compute(11)
    late = travel((3, 4, 5))
    forward(late, 1)
    forward(early, 9)
    for _ in range(12):
        forward(early, 1)
        forward(late, 1)
    forward(early, 60)
    forward(late, 60)
    last = remote(done, other_done, send.at[n, 0], recv.at[n, 0], partner)
    last.start()
    last.wait_recv()

    @pl.when(core == 0)
    def _():
        out_ref[:, :HALF] = done[0:20]
        out_ref[:, HALF:] = other_done[0:20]

    @pl.when(core == 1)
    def _():
        out_ref[:, :HALF] = other_done[20:40]
        out_ref[:, HALF:] = done[20:40]

    last.wait_send()
    for key, copy in copies.items():
        if key[1] != "far" or key[0] >= 3:
            copy.wait_send()


def finish(grad_gate, grad_up, pick, w_gate, w_up):
    full = [pltpu.VMEM((RING, RING, RING, ROWS, w), BF) for w in WIDTHS]
    lines = [pltpu.VMEM((RING, RING, ROWS, w), BF) for w in WIDTHS]
    line = [pltpu.VMEM((RING, ROWS, w), BF) for w in WIDTHS]
    cell = [pltpu.VMEM((ROWS, w), BF) for w in WIDTHS]
    hidden = w_gate.shape[1]
    return pl.pallas_call(
        finish_kernel,
        out_shape=jax.ShapeDtypeStruct((ROWS // 2, WIDTH), BF),
        in_specs=[pl.BlockSpec(memory_space=pltpu.VMEM)] * 3 + [pl.BlockSpec(memory_space=pl.ANY)] * 2,
        out_specs=pl.BlockSpec(memory_space=pltpu.VMEM),
        scratch_shapes=full * 2
        + lines * 3
        + line * 3
        + cell * 3
        + [
            pltpu.VMEM((3, RING, RING, RING, ROWS, WIDEST), BF),
            pltpu.VMEM((2, 2, 2, hidden, WIDEST), BF),
            pltpu.VMEM((RING * RING, 2, SLOTS, WIDEST), BF),
            pltpu.VMEM((ROWS, HALF), BF),
            pltpu.VMEM((ROWS, HALF), BF),
            pltpu.SemaphoreType.DMA((2, 2)),
            pltpu.SemaphoreType.DMA((STREAMS + 1, STREAM_COPIES)),
            pltpu.SemaphoreType.DMA((STREAMS + 1, STREAM_COPIES)),
        ],
        compiler_params=pltpu.CompilerParams(
            collective_id=1, has_side_effects=True, vmem_limit_bytes=60 * 1024 * 1024
        ),
        name="finish",
    )(grad_gate, grad_up, pick, w_gate, w_up)


def turned(a, b):
    return lax.dot_general(a, b, (((0,), (0,)), ((), ())), preferred_element_type=F32)


def select_kernel(group_ref, all_ref, x_ref, g_ref, pick_ref):
    info = all_ref[0, 0, :, WIDTH:]
    meta = info.astype(F32)
    row = lax.broadcasted_iota(jnp.int32, (GROUP, 1), 0)
    lane = lax.broadcasted_iota(jnp.int32, (GROUP, 128), 1)
    same = lax.broadcasted_iota(jnp.int32, (GROUP, GROUP), 0) % ROWS == (
        lax.broadcasted_iota(jnp.int32, (GROUP, GROUP), 1) % ROWS
    )
    total = jnp.dot(same.astype(F32).astype(BF), info, preferred_element_type=F32)[:, 9:10] * 0.0625
    reward = meta[:, 9:10] * 0.0625
    advantage = reward - (total - reward) / 3.0
    live = (row % 20).astype(F32) < meta[:, 8:9]
    weight = jnp.where(live, -advantage, 0.0)
    first = (2 * group_ref[0]).astype(F32)
    scale = jnp.zeros((128, 128), F32)
    pick = jnp.zeros((GROUP, 128), F32)
    for k in range(2):
        j = meta[:, k : k + 1] - first
        valid = (j >= 0.0) & (j < 2.0)
        slot = j * SLOTS + ((row // 20) * CAP).astype(F32) + meta[:, 10 + k : 11 + k]
        slot = jnp.where(valid, slot, -1.0).astype(jnp.int32)
        one = (lane == slot).astype(F32)
        pick = pick + one
        c = 2 + 3 * k
        value = ((meta[:, c : c + 1] + meta[:, c + 1 : c + 2]) + meta[:, c + 2 : c + 3]) * weight
        high = value.astype(BF).astype(F32)
        middle = (value - high).astype(BF).astype(F32)
        low = value - high - middle
        pieces = jnp.where(lane == 0, high, jnp.where(lane == 1, middle, jnp.where(lane == 2, low, 0.0)))
        scale = scale + turned(one.astype(BF), pieces.astype(BF))
    column = (scale[:, 0:1] + scale[:, 1:2]) + scale[:, 2:3]
    pick = pick.astype(BF)
    pick_ref[0] = pick
    for start in range(0, WIDTH, 1024):
        cols = slice(start, start + 1024)
        x = turned(pick, all_ref[0, 0, :, cols]).astype(BF)
        g = (turned(pick, all_ref[1, 0, :, cols]) * column).astype(BF)
        for j in range(2):
            x_ref[j, :, cols] = x[j * SLOTS : (j + 1) * SLOTS]
            g_ref[j, :, cols] = g[j * SLOTS : (j + 1) * SLOTS]


def select_rows(group, everything):
    blocks = everything.shape[1]
    rows = jax.ShapeDtypeStruct((2, blocks * SLOTS, WIDTH), BF)
    return pl.pallas_call(
        select_kernel,
        grid=(blocks,),
        out_shape=(rows, rows, jax.ShapeDtypeStruct((blocks, GROUP, 128), BF)),
        in_specs=[
            pl.BlockSpec(memory_space=pltpu.SMEM),
            pl.BlockSpec((2, 1, GROUP, WIDTH + META), lambda b: (0, b, 0, 0)),
        ],
        out_specs=(
            pl.BlockSpec((2, SLOTS, WIDTH), lambda b: (0, b, 0)),
            pl.BlockSpec((2, SLOTS, WIDTH), lambda b: (0, b, 0)),
            pl.BlockSpec((1, GROUP, 128), lambda b: (b, 0, 0)),
        ),
        name="select_rows",
    )(group, everything)


def three(values):
    high = lax.reduce_precision(values, 8, 7)
    middle = lax.reduce_precision(values - high, 8, 7)
    return [high, middle, values - high - middle]


def own_rows(tokens, cotangent, routes, gate_weights, lengths, rewards):
    count = tokens.shape[0]
    flat = routes.reshape(-1)
    before = jnp.arange(2 * count)[:, None] > jnp.arange(2 * count)[None, :]
    same = flat[:, None] == flat[None, :]
    earlier = jnp.sum((before & same).astype(jnp.int32), axis=1).reshape(count, 2)
    wide = jnp.ones((count, 1), F32)
    columns = [routes.astype(F32)]
    for k in range(2):
        columns += three(gate_weights[:, k : k + 1])
    columns += [wide * lengths[0, 0].astype(F32), wide * rewards[0, 0].astype(F32), earlier.astype(F32)]
    meta = jnp.concatenate(columns, axis=1)
    meta = jnp.pad(meta, ((0, 0), (0, META - meta.shape[1]))).astype(BF)
    return jnp.stack(
        [jnp.concatenate([tokens, meta], axis=1), jnp.concatenate([cotangent, jnp.zeros_like(meta)], axis=1)]
    )


def local(tokens, cotangent, routes, gate_weights, lengths, rewards, w_gate, w_up, w_down):
    own = own_rows(tokens, cotangent, routes, gate_weights, lengths, rewards)
    everything = gather_rows(own)
    everything = everything.reshape(2, RING * RING, GROUP, WIDTH + META)
    group = lax.axis_index("expert").astype(jnp.int32).reshape(1)
    x, g, pick = select_rows(group, everything)
    forward = functools.partial(jnp.einsum, "jcd,jfd->jcf", preferred_element_type=F32)
    weigh = functools.partial(jnp.einsum, "jcf,jcd->jfd", preferred_element_type=F32)
    pre_gate, pre_up, grad_hidden = forward(x, w_gate), forward(x, w_up), forward(g, w_down)
    prob = jax.nn.sigmoid(pre_gate)
    active = pre_gate * prob
    hidden = (active * pre_up).astype(BF)
    grad_gate = (grad_hidden * pre_up * (prob * (1.0 + pre_gate * (1.0 - prob)))).astype(BF)
    grad_up = (grad_hidden * active).astype(BF)
    grad_tokens = finish(grad_gate, grad_up, pick, w_gate, w_up)
    return (
        grad_tokens,
        weigh(grad_gate, x).astype(BF),
        weigh(grad_up, x).astype(BF),
        weigh(hidden, g).astype(BF),
    )


def solution(mesh):
    rows = P(("dp", "expert", "sample"), None)
    pair = P(("dp", "expert"), "sample")
    weights = P("expert", ("dp", "sample"), None)
    return jax.shard_map(
        local,
        mesh=mesh,
        in_specs=(rows,) * 4 + (pair,) * 2 + (weights,) * 3,
        out_specs=(rows,) + (weights,) * 3,
        check_vma=False,
    )
```

```python
import jax
import jax.numpy as jnp
from jax import lax
from jax.experimental import pallas as pl
from jax.experimental.pallas import tpu as pltpu
from jax.sharding import PartitionSpec as P

RING = 4
WIDTH = 4096
META = 128
ROWS = 40
MESH = pl.DeviceIdType.MESH
ORDERS = (("x", "y", "z"), ("y", "z", "x"), ("z", "x", "y"))
BF = jnp.bfloat16
F32 = jnp.float32


def place():
    dp = lax.axis_index("dp")
    ex = lax.axis_index("expert")
    return {"x": lax.axis_index("sample"), "y": (dp % 2) * 2 + ex // 2, "z": dp // 2}, ex % 2


def device(at, core):
    return {
        "dp": at["z"] * 2 + at["y"] // 2,
        "expert": (at["y"] % 2) * 2 + core,
        "sample": at["x"],
    }


def moved(at, axis, by):
    return {**at, axis: lax.rem(at[axis] + (by + RING), RING)}


def greet(at, core):
    barrier = pltpu.get_barrier_semaphore()
    peers = [device(moved(at, axis, by), core) for axis in "xyz" for by in (1, -1)]
    peers.append(device(at, 1 - core))
    for peer in peers:
        pl.semaphore_signal(barrier, inc=1, device_id=peer, device_id_type=MESH)
    pl.semaphore_wait(barrier, len(peers))


def remote(src, dst, send, recv, peer):
    return pltpu.make_async_remote_copy(
        src_ref=src, dst_ref=dst, send_sem=send, recv_sem=recv, device_id=peer, device_id_type=MESH
    )


class Plan:
    def __init__(self):
        self.now = 0.0
        self.free = {}
        self.ready = {}

    def send(self, key, lane, size):
        rate, delay = (5e5, 1.5) if lane == "pair" else (4.6e4, 2.8)
        end = max(self.now, self.free.get(lane, 0.0)) + size / rate
        self.free[lane] = end
        self.ready[key] = end + delay

    def mark(self, key, delay=0.0):
        self.ready[key] = self.now + delay

    def run(self, actors):
        waiting = [(actor, next(actor, None)) for actor in actors]
        while any(need is not None for _, need in waiting):
            best = None
            for i, (actor, need) in enumerate(waiting):
                if need is None or any(key not in self.ready for key in need[0]):
                    continue
                at = max([self.now] + [self.ready[key] for key in need[0]])
                if best is None or at < best[0]:
                    best = (at, i)
            at, i = best
            actor, need = waiting[i]
            self.now = at + need[1]
            waiting[i] = (actor, next(actor, None))


CHUNK_WIDTHS = (640, 512, 256)
CHUNK_STARTS = (0, 640, 1152)
PART = (WIDTH + META) // 3
GATHER_COPIES = 23
GROUP = RING * ROWS
TOKENS = RING * RING * GROUP
PLANE = RING * GROUP
UNITS = 256
BLOCKS = 6


def turned(a, b):
    return lax.dot_general(a, b, (((1,), (1,)), ((), ())), preferred_element_type=F32)


def gather_kernel(own_ref, wg_ref, wu_ref, wd_ref, out_ref, grad_ref, hidden_ref, *scratch):
    mate, block, total, tiles, weights, info, scales, keep, tsem, wsem, send, recv = scratch
    at, core = place()
    partner = device(at, 1 - core)
    plan = Plan()
    copies = {}
    settled = []
    greet(at, core)
    swap = remote(own_ref.at[1 - core], mate, send.at[9, 0], recv.at[9, 0], partner)
    swap.start()
    swap.wait()

    @pl.when(core == 0)
    def _():
        block[0:20] = own_ref[0]
        block[20:40] = mate[...]

    @pl.when(core == 1)
    def _():
        block[0:20] = mate[...]
        block[20:40] = own_ref[1]

    here = pltpu.make_async_copy(block, out_ref.at[core, at["z"], at["y"], pl.ds(pl.multiple_of(at["x"] * ROWS, 8), ROWS)], keep)
    here.start()

    def columns(s):
        return pl.ds((s % 3) * PART + CHUNK_STARTS[s // 3], CHUNK_WIDTHS[s // 3])

    def view(s, **over):
        to = {**at, **over}
        x = to["x"]
        if isinstance(x, pl.Slice):
            x = pl.ds(x.start * ROWS, x.size * ROWS)
        else:
            x = pl.ds(pl.multiple_of(x * ROWS, 8), ROWS)
        return out_ref.at[core, to["z"], to["y"], x, columns(s)]

    def push(s, k, src, dst, peer, lane, count):
        copy = remote(src, dst, send.at[s, k], recv.at[s, k], peer)
        copy.start()
        copies[s, k] = copy
        plan.send((s, k), lane, count * ROWS * CHUNK_WIDTHS[s // 3] * 2)

    def near(axis, by):
        return device(moved(at, axis, by), core)

    def coord(axis, by):
        return at[axis] if by == 0 else moved(at, axis, by)[axis]

    every = pl.ds(0, RING)
    offset = (0, -1, 1, 2)

    def line(s, l, plane=0):
        d1, d2, d3 = ORDERS[s % 3]
        return view(s, **{d1: every, d2: coord(d2, offset[l]), d3: coord(d3, plane)})

    def hand(s, n):
        d1, d2, d3 = ORDERS[s % 3]
        ref = view(s, **{d1: every, d2: every, d3: coord(d3, offset[n])})
        push(s, 19 + n, ref, ref, partner, "pair", 16)

    def travel(s):
        d1, d2, d3 = ORDERS[s % 3]
        tick = 0.05

        def along(k, ref, axis, by, count):
            push(s, k, ref, ref, near(axis, by), (axis, by), count)

        def spread(l):
            along(7 + 2 * l, line(s, l), d3, 1, 4)
            along(8 + 2 * l, line(s, l), d3, -1, 4)

        mine = block.at[:, columns(s)]
        for k, by in ((0, 1), (1, -1)):
            push(s, k, mine, view(s), near(d1, by), (d1, by), 1)
        yield [(s, 0)], tick
        copies[s, 0].wait_recv()
        along(2, view(s, **{d1: coord(d1, -1)}), d1, 1, 1)
        yield [(s, 1), (s, 2)], tick
        copies[s, 1].wait_recv()
        copies[s, 2].wait_recv()
        if not settled:
            here.wait()
            settled.append(True)
        along(3, line(s, 0), d2, 1, 4)
        along(4, line(s, 0), d2, -1, 4)
        spread(0)
        yield [(s, 3)], tick
        copies[s, 3].wait_recv()
        along(5, view(s, **{d1: pl.ds(0, 2), d2: coord(d2, -1)}), d2, 1, 2)
        spread(1)
        yield [(s, 4)], tick
        copies[s, 4].wait_recv()
        along(6, view(s, **{d1: pl.ds(2, 2), d2: coord(d2, 1)}), d2, -1, 2)
        spread(2)
        yield [(s, 5), (s, 6)], tick
        copies[s, 5].wait_recv()
        copies[s, 6].wait_recv()
        spread(3)
        hand(s, 0)
        for l in range(4):
            for k, by in ((0, 1), (1, -1)):
                yield [(s, 7 + 2 * l + k)], tick
                copies[s, 7 + 2 * l + k].wait_recv()
                if k == l // 2:
                    along(15 + l, line(s, l, -by), d3, by, 4)
        hand(s, 1)
        hand(s, 2)
        yield [(s, 15 + l) for l in range(4)], tick
        for l in range(4):
            copies[s, 15 + l].wait_recv()
        hand(s, 3)
        plan.mark(("all", s))

    def work():
        turn = 0
        for s in range(9):
            w = CHUNK_WIDTHS[s // 3]
            yield [("all", s)] + [(s, 19 + n) for n in range(4)], 0.1
            for n in range(4):
                copies[s, 19 + n].wait_recv()
            lead = META if s == 0 else 0
            loads = []
            start = (s % 3) * PART + CHUNK_STARTS[s // 3] - META + lead
            sources = ((wg_ref, 0), (wu_ref, 0), (wg_ref, 1), (wu_ref, 1), (wd_ref, 0), (wd_ref, 1))
            for k, (ref, j) in enumerate(sources):
                to = weights.at[k, :, pl.ds(lead, w - lead)]
                loads.append(pltpu.make_async_copy(ref.at[j, :, pl.ds(start, w - lead)], to, wsem.at[k]))

            def fetch(half):
                got = []
                for a in range(2):
                    src = out_ref.at[a, pl.ds(2 * half, 2), :, :, columns(s)]
                    got.append(pltpu.make_async_copy(src, tiles.at[half, a, :, :, :, pl.ds(0, w)], tsem.at[half, a]))
                return got

            loads += fetch(0)
            if s == 0:
                loads.append(pltpu.make_async_copy(out_ref.at[0, :, :, :, pl.ds(0, META)], info, keep))
                weights[:, :, :META] = jnp.zeros((BLOCKS, UNITS, META), BF)
            later = fetch(1)
            for copy in loads + later:
                copy.start()
            plan.mark(("load", s), 2.5)
            yield [("load", s)], 4.0 * w / 640
            for half in range(2):
                if half:
                    yield [], 4.0 * w / 640
                for copy in later if half else loads:
                    copy.wait()

                def body(i, carry):
                    z, pair = i // 3, i % 3
                    tile = tiles[half, pair // 2, z, :, :, :w].reshape(PLANE, w)
                    where = pl.ds(pl.multiple_of((2 * half + z) * PLANE, 8), PLANE)
                    for k in range(2):
                        q = pair * 2 + k
                        value = turned(tile, weights[q, :, :w])
                        if s == 0:
                            total[q, where, :] = value
                        else:
                            total[q, where, :] += value
                    return carry

                lax.fori_loop(0, 6, body, 0)

    plan.run([travel(s) for s in range(9)] + [work()])

    first = (2 * lax.axis_index("expert")).astype(F32)
    same = (
        lax.broadcasted_iota(jnp.int32, (GROUP, GROUP), 0) % ROWS
        == lax.broadcasted_iota(jnp.int32, (GROUP, GROUP), 1) % ROWS
    ).astype(F32).astype(BF)

    def scale(i, carry):
        rows = info[i // RING, i % RING]
        meta = rows.astype(F32)
        reward = meta[:, 9:10] * 0.0625
        all_rewards = jnp.dot(same, rows, preferred_element_type=F32)[:, 9:10] * 0.0625
        advantage = reward - (all_rewards - reward) / 3.0
        position = lax.broadcasted_iota(jnp.int32, (GROUP, 1), 0) % 20
        weight = jnp.where(position.astype(F32) < meta[:, 8:9], -advantage, 0.0)
        lane = lax.broadcasted_iota(jnp.int32, (GROUP, 128), 1).astype(F32)
        value = jnp.zeros((GROUP, 128), F32)
        for k in range(2):
            c = 2 + 3 * k
            pair = ((meta[:, c : c + 1] + meta[:, c + 1 : c + 2]) + meta[:, c + 2 : c + 3]) * weight
            value = jnp.where(lane == meta[:, k : k + 1] - first, pair, value)
        scales[pl.ds(pl.multiple_of(i * GROUP, 8), GROUP), :] = value
        return carry

    lax.fori_loop(0, RING * RING, scale, 0)

    def activate(i, carry):
        where = pl.ds(pl.multiple_of(i * 128, 128), 128)
        for j in range(2):
            pre_gate, pre_up = total[2 * j, where, :], total[2 * j + 1, where, :]
            by = scales[where, j : j + 1]
            grad_hidden = total[4 + j, where, :] * by
            prob = 1.0 / (1.0 + jnp.exp(-pre_gate))
            active = pre_gate * prob
            slope = prob * (1.0 + pre_gate * (1.0 - prob))
            grad_ref[where, 2 * j * UNITS : (2 * j + 1) * UNITS] = (grad_hidden * pre_up * slope).astype(BF)
            grad_ref[where, (2 * j + 1) * UNITS : (2 * j + 2) * UNITS] = (grad_hidden * active).astype(BF)
            hidden_ref[where, j * UNITS : (j + 1) * UNITS] = (active * pre_up * by).astype(BF)
        return carry

    lax.fori_loop(0, TOKENS // 128, activate, 0)
    for copy in copies.values():
        copy.wait_send()


def gather_rows(own, w_gate, w_up, w_down):
    anywhere = pl.BlockSpec(memory_space=pl.ANY)
    inside = pl.BlockSpec(memory_space=pltpu.VMEM)
    return pl.pallas_call(
        gather_kernel,
        out_shape=(
            jax.ShapeDtypeStruct((2, RING, RING, GROUP, WIDTH + META), BF),
            jax.ShapeDtypeStruct((TOKENS, 4 * UNITS), BF),
            jax.ShapeDtypeStruct((TOKENS, 2 * UNITS), BF),
        ),
        in_specs=[inside] + [anywhere] * 3,
        out_specs=(anywhere, inside, inside),
        scratch_shapes=[
            pltpu.VMEM((ROWS // 2, WIDTH + META), BF),
            pltpu.VMEM((ROWS, WIDTH + META), BF),
            pltpu.VMEM((BLOCKS, TOKENS, UNITS), F32),
            pltpu.VMEM((2, 2, 2, RING, GROUP, CHUNK_WIDTHS[0]), BF),
            pltpu.VMEM((BLOCKS, UNITS, CHUNK_WIDTHS[0]), BF),
            pltpu.VMEM((RING, RING, GROUP, META), BF),
            pltpu.VMEM((TOKENS, 128), F32),
            pltpu.SemaphoreType.DMA,
            pltpu.SemaphoreType.DMA((2, 2)),
            pltpu.SemaphoreType.DMA((BLOCKS,)),
            pltpu.SemaphoreType.DMA((10, GATHER_COPIES)),
            pltpu.SemaphoreType.DMA((10, GATHER_COPIES)),
        ],
        compiler_params=pltpu.CompilerParams(
            collective_id=0, has_side_effects=True, vmem_limit_bytes=60 * 1024 * 1024
        ),
        name="gather_rows",
    )(own, w_gate, w_up, w_down)


HALF = WIDTH // 2
WIDTHS = (384, 384, 256, 384, 256, 384)
STARTS = (0, 384, 768, 1024, 1408, 1664)
WIDEST = 384
STREAMS = 6
STREAM_COPIES = 22
AHEAD = (3, 1)
BEHIND = (2, 0)


def finish_kernel(grad_ref, hidden_ref, rows_ref, wg_ref, wu_ref, out_ref, dg_ref, du_ref, dd_ref, *scratch):
    n = STREAMS
    acc, mate, fa, ma, pa, fb, mb, pb, fc, mc, pc = [scratch[n * i : n * i + n] for i in range(11)]
    give, weights, done, other_done, across, tiles, made, some, wsem, tsem, msem, hsem, send, recv = scratch[11 * n :]
    plan = Plan()
    at, core = place()
    partner = device(at, 1 - core)
    copies = {}
    every = pl.ds(0, RING)
    offset = (0, -1, 1, 2)

    def near(axis, by):
        return device(moved(at, axis, by), core)

    def coord(axis, by):
        return at[axis] if by == 0 else moved(at, axis, by)[axis]

    def spot(**over):
        to = {**at, **over}
        return to["z"], to["y"], to["x"]

    def order(s):
        return ORDERS[s % 3]

    def push(s, key, k, src, dst, peer, lane, count):
        copy = remote(src, dst, send.at[s, k], recv.at[s, k], peer)
        copy.start()
        copies[(s,) + key] = copy
        plan.send((s,) + key, lane, count * ROWS * WIDTHS[s] * 2)

    def along(s, key, k, src, dst, axis, by, count):
        push(s, key, k, src, dst, near(axis, by), (axis, by), count)

    turns = [(s, far) for c in (0, 3) for far in (True, False) for s in range(c, c + 3)]

    def fetch(turn):
        s, far = turns[turn]
        side = 1 - core if far else core
        columns = pl.ds(pl.multiple_of(side * HALF + STARTS[s], 128), WIDTHS[s])
        got = []
        for q in range(4):
            ref = (wg_ref, wu_ref)[q % 2].at[q // 2, :, columns]
            to = weights.at[turn % 2, q, :, pl.ds(0, WIDTHS[s])]
            got.append(pltpu.make_async_copy(ref, to, wsem.at[turn % 2, q]))
            got[-1].start()
        return got

    fetched = {0: fetch(0)}

    def compute(turn):
        s, far = turns[turn]
        w = WIDTHS[s]
        slot = turn % 2
        if turn + 1 < len(turns):
            fetched[turn + 1] = fetch(turn + 1)
        for copy in fetched[turn]:
            copy.wait()
        if far:
            if s >= 3:
                copies[s - 3, "far"].wait_send()
        else:
            copies[s, "far"].wait_recv()

        def rows_of(z, carry):
            take = pl.ds(pl.multiple_of(z * PLANE, 8), PLANE)
            total = jnp.dot(grad_ref[take, :UNITS], weights[slot, 0, :, :w], preferred_element_type=F32)
            for q in range(1, 4):
                total += jnp.dot(
                    grad_ref[take, q * UNITS : (q + 1) * UNITS], weights[slot, q, :, :w], preferred_element_type=F32
                )
            for i in range(RING * RING):
                y, x = i // RING, i % RING
                piece = total[i * ROWS : (i + 1) * ROWS]
                if far:
                    give[s % 3, z, y, x, :, :w] = piece.astype(BF)
                else:
                    acc[s][z, y, x] = (piece + mate[s][z, y, x].astype(F32)).astype(BF)
            return carry

        lax.fori_loop(0, RING, rows_of, 0)
        if far:
            push(s, ("far",), 21, give.at[s % 3, :, :, :, :, pl.ds(0, w)], mate[s], partner, "pair", 64)
        else:
            plan.mark(("own", s))

    def add(dst, index, *terms):
        total = dst[index].astype(F32)
        for ref, where in terms:
            total = total + ref[where].astype(F32)
        dst[index] = total.astype(BF)

    def line(s, r, by):
        d1, d2, d3 = order(s)
        return acc[s].at[spot(**{d1: every, d2: coord(d2, offset[r]), d3: coord(d3, by)})]

    def add_line(s, r, by, *terms, first=0, count=RING):
        d1, d2, d3 = order(s)

        def body(i, carry):
            where = spot(**{d1: i, d2: coord(d2, offset[r]), d3: coord(d3, by)})
            add(acc[s], where, *[(ref, (r, i) if lead else (i,)) for ref, lead in terms])
            return carry

        lax.fori_loop(first, first + count, body, 0)

    def piece(s, r, half):
        d1, d2, d3 = order(s)
        return acc[s].at[spot(**{d1: pl.ds(2 * half, 2), d2: coord(d2, offset[r])})]

    def half_of(ref, half):
        return ref.at[pl.ds(2 * half, 2)]

    def cell(s, by):
        d1 = order(s)[0]
        return spot(**{d1: coord(d1, by)})

    def travel(s):
        d1, d2, d3 = order(s)
        cost = 0.3
        yield [("own", s)], 0.1
        for r in (3, 2, 1, 0):
            along(s, ("fa", r), r, line(s, r, 2), fa[s].at[r], d3, 1 if r in AHEAD else -1, 4)
        for r in BEHIND:
            along(s, ("ma", r), 4 + r, line(s, r, 1), ma[s].at[r], d3, 1, 4)
        for r in AHEAD:
            along(s, ("pa", r), 8 + r, line(s, r, -1), pa[s].at[r], d3, -1, 4)
        for r in (3, 2, 1, 0):
            yield [(s, "fa", r)], cost
            copies[s, "fa", r].wait_recv()
            if r in AHEAD:
                add_line(s, r, 1, (fa[s], True))
                along(s, ("ma", r), 4 + r, line(s, r, 1), ma[s].at[r], d3, 1, 4)
            else:
                add_line(s, r, -1, (fa[s], True))
                along(s, ("pa", r), 8 + r, line(s, r, -1), pa[s].at[r], d3, -1, 4)
        for r in (3, 2, 1, 0):
            yield [(s, "ma", r), (s, "pa", r)], cost
            copies[s, "ma", r].wait_recv()
            copies[s, "pa", r].wait_recv()
            add_line(s, r, 0, (ma[s], True), (pa[s], True))
            if r == 3:
                along(s, ("fb", 0), 12, piece(s, 3, 0), half_of(fb[s], 0), d2, 1, 2)
                along(s, ("fb", 1), 13, piece(s, 3, 1), half_of(fb[s], 1), d2, -1, 2)
            if r == 2:
                along(s, ("mb", 1), 15, piece(s, 2, 1), half_of(mb[s], 1), d2, 1, 2)
            if r == 1:
                along(s, ("pb", 0), 16, piece(s, 1, 0), half_of(pb[s], 0), d2, -1, 2)
        yield [(s, "fb", 0)], cost
        copies[s, "fb", 0].wait_recv()
        add_line(s, 2, 0, (fb[s], False), first=0, count=2)
        along(s, ("mb", 0), 14, piece(s, 2, 0), half_of(mb[s], 0), d2, 1, 2)
        yield [(s, "fb", 1)], cost
        copies[s, "fb", 1].wait_recv()
        add_line(s, 1, 0, (fb[s], False), first=2, count=2)
        along(s, ("pb", 1), 17, piece(s, 1, 1), half_of(pb[s], 1), d2, -1, 2)
        yield [(s, key, half) for key in ("mb", "pb") for half in (0, 1)], cost
        for half in (0, 1):
            copies[s, "mb", half].wait_recv()
            copies[s, "pb", half].wait_recv()
        add_line(s, 0, 0, (mb[s], False), (pb[s], False))
        along(s, ("fc",), 18, acc[s].at[cell(s, 2)], fc[s], d1, 1, 1)
        along(s, ("pc",), 20, acc[s].at[cell(s, -1)], pc[s], d1, -1, 1)
        yield [(s, "fc")], 0.1
        copies[s, "fc"].wait_recv()
        add(acc[s], cell(s, 1), (fc[s], ...))
        along(s, ("mc",), 19, acc[s].at[cell(s, 1)], mc[s], d1, 1, 1)
        yield [(s, "pc"), (s, "mc")], 0.1
        copies[s, "pc"].wait_recv()
        copies[s, "mc"].wait_recv()
        own = acc[s][cell(s, 0)].astype(F32) + pc[s][...].astype(F32) + mc[s][...].astype(F32)
        done[:, STARTS[s] : STARTS[s] + WIDTHS[s]] = own.astype(BF)
        plan.mark(("end", s))
        yield [("end", s)], 0.0

    def produce():
        for turn, (s, far) in enumerate(turns):
            yield [] if far else [(s, "far")], 3.0 * WIDTHS[s] / 384
            compute(turn)
        plan.mark("produced")

    def weigh():
        yield ["produced"], 0.2

        def load(t):
            got = []
            for a in range(2):
                src = rows_ref.at[a, :, pl.ds(META + t * UNITS, UNITS)]
                got.append(pltpu.make_async_copy(src, tiles.at[t % 2, a], tsem.at[t % 2, a]))
                got[-1].start()
            return got

        loaded = {0: load(0)}
        fetch_hidden = pltpu.make_async_copy(hidden_ref, some, hsem)
        fetch_hidden.start()
        for step in range(2):
            yield [], 5.0 if step == 0 else 2.5
            if step:
                fetch_hidden.wait()

            def turn_over(i, carry):
                where = pl.ds(pl.multiple_of(i * UNITS, UNITS), UNITS)
                for q in range(2 if step else 4):
                    src = (some if step else grad_ref)[where, q * UNITS : (q + 1) * UNITS]
                    across[4 * step + q, :, where] = src.T
                return carry

            lax.fori_loop(0, TOKENS // UNITS, turn_over, 0)
        stored = {}
        for t in range(WIDTH // UNITS):
            yield [], 2.6
            if t + 1 < WIDTH // UNITS:
                loaded[t + 1] = load(t + 1)
            for copy in loaded[t] + stored.pop(t - 2, []):
                copy.wait()

            def body(q, carry):
                value = jnp.dot(across[q], tiles[t % 2, q // 4], preferred_element_type=F32)
                made[t % 2, q] = value.astype(BF)
                return carry

            lax.fori_loop(0, BLOCKS, body, 0)
            stored[t] = []
            for q in range(BLOCKS):
                ref, j = ((dg_ref, du_ref)[q % 2], q // 2) if q < 4 else (dd_ref, q - 4)
                to = ref.at[j, :, pl.ds(t * UNITS, UNITS)]
                stored[t].append(pltpu.make_async_copy(made.at[t % 2, q], to, msem.at[t % 2, q]))
                stored[t][-1].start()
        for some_copies in stored.values():
            for copy in some_copies:
                copy.wait()

    greet(at, core)
    plan.run([travel(s) for s in range(n)] + [produce(), weigh()])
    last = remote(done, other_done, send.at[n, 0], recv.at[n, 0], partner)
    last.start()
    last.wait_recv()

    @pl.when(core == 0)
    def _():
        out_ref[:, :HALF] = done[0:20]
        out_ref[:, HALF:] = other_done[0:20]

    @pl.when(core == 1)
    def _():
        out_ref[:, :HALF] = other_done[20:40]
        out_ref[:, HALF:] = done[20:40]

    last.wait_send()
    for key, copy in copies.items():
        if key[1] != "far" or key[0] >= 3:
            copy.wait_send()


def finish(grads, hidden, rows, w_gate, w_up):
    full = [pltpu.VMEM((RING, RING, RING, ROWS, w), BF) for w in WIDTHS]
    lines = [pltpu.VMEM((RING, RING, ROWS, w), BF) for w in WIDTHS]
    line = [pltpu.VMEM((RING, ROWS, w), BF) for w in WIDTHS]
    cell = [pltpu.VMEM((ROWS, w), BF) for w in WIDTHS]
    anywhere = pl.BlockSpec(memory_space=pl.ANY)
    inside = pl.BlockSpec(memory_space=pltpu.VMEM)
    return pl.pallas_call(
        finish_kernel,
        out_shape=(jax.ShapeDtypeStruct((ROWS // 2, WIDTH), BF),) + (jax.ShapeDtypeStruct(w_gate.shape, BF),) * 3,
        in_specs=[inside] + [anywhere] * 4,
        out_specs=(inside,) + (anywhere,) * 3,
        scratch_shapes=full * 2
        + lines * 3
        + line * 3
        + cell * 3
        + [
            pltpu.VMEM((3, RING, RING, RING, ROWS, WIDEST), BF),
            pltpu.VMEM((2, 4, UNITS, WIDEST), BF),
            pltpu.VMEM((ROWS, HALF), BF),
            pltpu.VMEM((ROWS, HALF), BF),
            pltpu.VMEM((BLOCKS, UNITS, TOKENS), BF),
            pltpu.VMEM((2, 2, TOKENS, UNITS), BF),
            pltpu.VMEM((2, BLOCKS, UNITS, UNITS), BF),
            pltpu.VMEM((TOKENS, 2 * UNITS), BF),
            pltpu.SemaphoreType.DMA((2, 4)),
            pltpu.SemaphoreType.DMA((2, 2)),
            pltpu.SemaphoreType.DMA((2, BLOCKS)),
            pltpu.SemaphoreType.DMA,
            pltpu.SemaphoreType.DMA((STREAMS + 1, STREAM_COPIES)),
            pltpu.SemaphoreType.DMA((STREAMS + 1, STREAM_COPIES)),
        ],
        compiler_params=pltpu.CompilerParams(
            collective_id=1, has_side_effects=True, vmem_limit_bytes=67000000
        ),
        name="finish",
    )(grads, hidden, rows, w_gate, w_up)


def three(values):
    high = lax.reduce_precision(values, 8, 7)
    middle = lax.reduce_precision(values - high, 8, 7)
    return [high, middle, values - high - middle]


def own_rows(tokens, cotangent, routes, gate_weights, lengths, rewards):
    count = tokens.shape[0]
    wide = jnp.ones((count, 1), F32)
    columns = [routes.astype(F32)]
    for k in range(2):
        columns += three(gate_weights[:, k : k + 1])
    columns += [wide * lengths[0, 0].astype(F32), wide * rewards[0, 0].astype(F32)]
    meta = jnp.concatenate(columns, axis=1)
    meta = jnp.pad(meta, ((0, 0), (0, META - meta.shape[1]))).astype(BF)
    return jnp.stack(
        [jnp.concatenate([meta, tokens], axis=1), jnp.concatenate([jnp.zeros_like(meta), cotangent], axis=1)]
    )


def local(tokens, cotangent, routes, gate_weights, lengths, rewards, w_gate, w_up, w_down):
    own = own_rows(tokens, cotangent, routes, gate_weights, lengths, rewards)
    everything, grads, hidden = gather_rows(own, w_gate, w_up, w_down)
    everything = everything.reshape(2, TOKENS, WIDTH + META)
    return finish(grads, hidden, everything, w_gate, w_up)


def solution(mesh):
    rows = P(("dp", "expert", "sample"), None)
    pair = P(("dp", "expert"), "sample")
    weights = P("expert", ("dp", "sample"), None)
    return jax.shard_map(
        local,
        mesh=mesh,
        in_specs=(rows,) * 4 + (pair,) * 2 + (weights,) * 3,
        out_specs=(rows,) + (weights,) * 3,
        check_vma=False,
    )
```

```python
import jax
import jax.numpy as jnp
from jax import lax
from jax.experimental import pallas as pl
from jax.experimental.pallas import tpu as pltpu
from jax.sharding import PartitionSpec as P

RING = 4
WIDTH = 4096
META = 128
ROWS = 40
MESH = pl.DeviceIdType.MESH
ORDERS = (("x", "y", "z"), ("y", "z", "x"), ("z", "x", "y"))
BF = jnp.bfloat16
F32 = jnp.float32


def place():
    dp = lax.axis_index("dp")
    ex = lax.axis_index("expert")
    return {"x": lax.axis_index("sample"), "y": (dp % 2) * 2 + ex // 2, "z": dp // 2}, ex % 2


def device(at, core):
    return {
        "dp": at["z"] * 2 + at["y"] // 2,
        "expert": (at["y"] % 2) * 2 + core,
        "sample": at["x"],
    }


def moved(at, axis, by):
    return {**at, axis: lax.rem(at[axis] + (by + RING), RING)}


def greet(at, core):
    barrier = pltpu.get_barrier_semaphore()
    peers = [device(moved(at, axis, by), core) for axis in "xyz" for by in (1, -1)]
    peers.append(device(at, 1 - core))
    for peer in peers:
        pl.semaphore_signal(barrier, inc=1, device_id=peer, device_id_type=MESH)
    pl.semaphore_wait(barrier, len(peers))


def remote(src, dst, send, recv, peer):
    return pltpu.make_async_remote_copy(
        src_ref=src, dst_ref=dst, send_sem=send, recv_sem=recv, device_id=peer, device_id_type=MESH
    )


class Plan:
    def __init__(self, delay, slack):
        self.delay = delay
        self.slack = slack
        self.now = 0.0
        self.free = {}
        self.ready = {}

    def send(self, key, lane, size):
        rate, delay = (5e5, 1.5) if lane == "pair" else (4.6e4, self.delay)
        end = max(self.now, self.free.get(lane, 0.0)) + size / rate
        self.free[lane] = end
        self.ready[key] = end + delay

    def mark(self, key, delay=0.0):
        self.ready[key] = self.now + delay

    def run(self, actors):
        waiting = [(actor, next(actor, None)) for actor in actors]
        while any(need is not None for _, need in waiting):
            best = None
            for i, (actor, need) in enumerate(waiting):
                if need is None or any(key not in self.ready for key in need[0]):
                    continue
                queued = [self.free.get(lane, 0.0) - self.slack for lane in need[2:]]
                at = max([self.now] + [self.ready[key] for key in need[0]] + queued)
                if best is None or at < best[0]:
                    best = (at, i)
            at, i = best
            actor, need = waiting[i]
            self.now = at + need[1]
            waiting[i] = (actor, next(actor, None))


CHUNK_WIDTHS = (512, 640, 256)
CHUNK_STARTS = (0, 512, 1152)
PART = (WIDTH + META) // 3
GATHER_COPIES = 23
GROUP = RING * ROWS
TOKENS = RING * RING * GROUP
PLANE = RING * GROUP
UNITS = 256
BLOCKS = 6


def turned(a, b):
    return lax.dot_general(a, b, (((1,), (1,)), ((), ())), preferred_element_type=F32)


def gather_kernel(own_ref, wg_ref, wu_ref, wd_ref, out_ref, grad_ref, hidden_ref, *scratch):
    mate, block, total, tiles, weights, info, scales, keep, tsem, wsem, send, recv = scratch
    at, core = place()
    partner = device(at, 1 - core)
    plan = Plan(3.4, 5.0)
    copies = {}
    settled = []
    greet(at, core)
    swap = remote(own_ref.at[1 - core], mate, send.at[9, 0], recv.at[9, 0], partner)
    swap.start()
    swap.wait()

    @pl.when(core == 0)
    def _():
        block[0:20] = own_ref[0]
        block[20:40] = mate[...]

    @pl.when(core == 1)
    def _():
        block[0:20] = mate[...]
        block[20:40] = own_ref[1]

    here = pltpu.make_async_copy(block, out_ref.at[core, at["z"], at["y"], pl.ds(pl.multiple_of(at["x"] * ROWS, 8), ROWS)], keep)
    here.start()

    def columns(s):
        return pl.ds((s % 3) * PART + CHUNK_STARTS[s // 3], CHUNK_WIDTHS[s // 3])

    def view(s, **over):
        to = {**at, **over}
        x = to["x"]
        if isinstance(x, pl.Slice):
            x = pl.ds(x.start * ROWS, x.size * ROWS)
        else:
            x = pl.ds(pl.multiple_of(x * ROWS, 8), ROWS)
        return out_ref.at[core, to["z"], to["y"], x, columns(s)]

    def push(s, k, src, dst, peer, lane, count):
        copy = remote(src, dst, send.at[s, k], recv.at[s, k], peer)
        copy.start()
        copies[s, k] = copy
        plan.send((s, k), lane, count * ROWS * CHUNK_WIDTHS[s // 3] * 2)

    def near(axis, by):
        return device(moved(at, axis, by), core)

    def coord(axis, by):
        return at[axis] if by == 0 else moved(at, axis, by)[axis]

    every = pl.ds(0, RING)
    offset = (0, -1, 1, 2)

    def line(s, l, plane=0):
        d1, d2, d3 = ORDERS[s % 3]
        return view(s, **{d1: every, d2: coord(d2, offset[l]), d3: coord(d3, plane)})

    def hand(s, n):
        d1, d2, d3 = ORDERS[s % 3]
        ref = view(s, **{d1: every, d2: every, d3: coord(d3, offset[n])})
        push(s, 19 + n, ref, ref, partner, "pair", 16)

    def travel(s):
        d1, d2, d3 = ORDERS[s % 3]
        tick = 0.05

        def along(k, ref, axis, by, count):
            push(s, k, ref, ref, near(axis, by), (axis, by), count)

        def spread(l):
            along(7 + 2 * l, line(s, l), d3, 1, 4)
            along(8 + 2 * l, line(s, l), d3, -1, 4)

        mine = block.at[:, columns(s)]
        for k, by in ((0, 1), (1, -1)):
            push(s, k, mine, view(s), near(d1, by), (d1, by), 1)
        ahead = lambda *axes: [(axis, by) for axis in axes for by in (1, -1)] if s >= 3 else []
        yield [(s, 0)], tick, *ahead(d1)
        copies[s, 0].wait_recv()
        along(2, view(s, **{d1: coord(d1, -1)}), d1, 1, 1)
        yield [(s, 1), (s, 2)], tick, *ahead(d2)
        copies[s, 1].wait_recv()
        copies[s, 2].wait_recv()
        if not settled:
            here.wait()
            settled.append(True)
        along(3, line(s, 0), d2, 1, 4)
        along(4, line(s, 0), d2, -1, 4)
        yield [], tick, (d3, 1), (d3, -1)
        spread(0)
        yield [(s, 3)], tick
        copies[s, 3].wait_recv()
        along(5, view(s, **{d1: pl.ds(0, 2), d2: coord(d2, -1)}), d2, 1, 2)
        yield [(s, 4)], tick
        copies[s, 4].wait_recv()
        along(6, view(s, **{d1: pl.ds(2, 2), d2: coord(d2, 1)}), d2, -1, 2)
        for l in (1, 2):
            yield [], tick, (d3, 1), (d3, -1)
            spread(l)
        yield [(s, 5), (s, 6)], tick
        copies[s, 5].wait_recv()
        copies[s, 6].wait_recv()
        spread(3)
        hand(s, 0)
        for l in range(4):
            for k, by in ((0, 1), (1, -1)):
                yield [(s, 7 + 2 * l + k)], tick
                copies[s, 7 + 2 * l + k].wait_recv()
                if k == l // 2:
                    along(15 + l, line(s, l, -by), d3, by, 4)
        hand(s, 1)
        hand(s, 2)
        yield [(s, 15 + l) for l in range(4)], tick
        for l in range(4):
            copies[s, 15 + l].wait_recv()
        hand(s, 3)
        plan.mark(("all", s))

    first = (2 * lax.axis_index("expert")).astype(F32)
    same = (
        lax.broadcasted_iota(jnp.int32, (GROUP, GROUP), 0) % ROWS
        == lax.broadcasted_iota(jnp.int32, (GROUP, GROUP), 1) % ROWS
    ).astype(F32).astype(BF)

    def scale(i, carry):
        rows = info[i // RING, i % RING]
        meta = rows.astype(F32)
        reward = meta[:, 9:10] * 0.0625
        all_rewards = jnp.dot(same, rows, preferred_element_type=F32)[:, 9:10] * 0.0625
        advantage = reward - (all_rewards - reward) / 3.0
        position = lax.broadcasted_iota(jnp.int32, (GROUP, 1), 0) % 20
        weight = jnp.where(position.astype(F32) < meta[:, 8:9], -advantage, 0.0)
        lane = lax.broadcasted_iota(jnp.int32, (GROUP, 128), 1).astype(F32)
        value = jnp.zeros((GROUP, 128), F32)
        for k in range(2):
            c = 2 + 3 * k
            pair = ((meta[:, c : c + 1] + meta[:, c + 1 : c + 2]) + meta[:, c + 2 : c + 3]) * weight
            value = jnp.where(lane == meta[:, k : k + 1] - first, pair, value)
        scales[pl.ds(pl.multiple_of(i * GROUP, 8), GROUP), :] = value
        return carry

    pending = {}

    def needs(s):
        return [("all", s)] + [(s, 19 + n) for n in range(4)]

    def begin(s):
        w = CHUNK_WIDTHS[s // 3]
        for n in range(4):
            copies[s, 19 + n].wait_recv()
        lead = META if s == 0 else 0
        start = (s % 3) * PART + CHUNK_STARTS[s // 3] - META + lead
        slot = s % 2
        loads = [[], []]
        sources = ((wg_ref, 0), (wu_ref, 0), (wg_ref, 1), (wu_ref, 1), (wd_ref, 0), (wd_ref, 1))
        for k, (ref, j) in enumerate(sources):
            to = weights.at[slot, k, :, pl.ds(lead, w - lead)]
            loads[0].append(pltpu.make_async_copy(ref.at[j, :, pl.ds(start, w - lead)], to, wsem.at[slot, k]))
        for half in range(2):
            for a in range(2):
                src = out_ref.at[a, pl.ds(2 * half, 2), :, :, columns(s)]
                to = tiles.at[slot, half, a, :, :, :, pl.ds(0, w)]
                loads[half].append(pltpu.make_async_copy(src, to, tsem.at[slot, half, a]))
        if s == 0:
            loads[0].append(pltpu.make_async_copy(out_ref.at[0, :, :, :, pl.ds(0, META)], info, keep))
            weights[0, :, :, :META] = jnp.zeros((BLOCKS, UNITS, META), BF)
        for half in range(2):
            for copy in loads[half]:
                copy.start()
        pending[s] = loads
        plan.mark(("load", s), 2.5)

    def work():
        for s in range(9):
            w = CHUNK_WIDTHS[s // 3]
            cost = {640: 2.7, 512: 2.2, 384: 2.0, 256: 1.7}[w]
            if s not in pending:
                yield needs(s), 0.1
                begin(s)
            for half in range(2):
                yield [("load", s)], cost
                for copy in pending[s][half]:
                    copy.wait()

                def body(i, carry):
                    z, pair = i // 3, i % 3
                    tile = tiles[s % 2, half, pair // 2, z, :, :, :w].reshape(PLANE, w)
                    where = pl.ds(pl.multiple_of((2 * half + z) * PLANE, 8), PLANE)
                    for k in range(2):
                        q = pair * 2 + k
                        value = turned(tile, weights[s % 2, q, :, :w])
                        if s == 0:
                            total[q, where, :] = value
                        else:
                            total[q, where, :] += value
                    return carry

                lax.fori_loop(0, 6, body, 0)
                if half == 0 and s < 8 and all(plan.ready.get(key, 1e9) <= plan.now for key in needs(s + 1)):
                    begin(s + 1)
            if s == 0:
                yield [], 4.2
                lax.fori_loop(0, RING * RING, scale, 0)

    plan.run([travel(s) for s in range(9)] + [work()])

    def activate(i, carry):
        where = pl.ds(pl.multiple_of(i * 128, 128), 128)
        for j in range(2):
            pre_gate, pre_up = total[2 * j, where, :], total[2 * j + 1, where, :]
            by = scales[where, j : j + 1]
            grad_hidden = total[4 + j, where, :] * by
            prob = 1.0 / (1.0 + jnp.exp(-pre_gate))
            active = pre_gate * prob
            slope = prob * (1.0 + pre_gate * (1.0 - prob))
            grad_ref[where, 2 * j * UNITS : (2 * j + 1) * UNITS] = (grad_hidden * pre_up * slope).astype(BF)
            grad_ref[where, (2 * j + 1) * UNITS : (2 * j + 2) * UNITS] = (grad_hidden * active).astype(BF)
            hidden_ref[where, j * UNITS : (j + 1) * UNITS] = (active * pre_up * by).astype(BF)
        return carry

    lax.fori_loop(0, TOKENS // 128, activate, 0)
    for copy in copies.values():
        copy.wait_send()


def gather_rows(own, w_gate, w_up, w_down):
    anywhere = pl.BlockSpec(memory_space=pl.ANY)
    inside = pl.BlockSpec(memory_space=pltpu.VMEM)
    return pl.pallas_call(
        gather_kernel,
        out_shape=(
            jax.ShapeDtypeStruct((2, RING, RING, GROUP, WIDTH + META), BF),
            jax.ShapeDtypeStruct((TOKENS, 4 * UNITS), BF),
            jax.ShapeDtypeStruct((TOKENS, 2 * UNITS), BF),
        ),
        in_specs=[inside] + [anywhere] * 3,
        out_specs=(anywhere, inside, inside),
        scratch_shapes=[
            pltpu.VMEM((ROWS // 2, WIDTH + META), BF),
            pltpu.VMEM((ROWS, WIDTH + META), BF),
            pltpu.VMEM((BLOCKS, TOKENS, UNITS), F32),
            pltpu.VMEM((2, 2, 2, 2, RING, GROUP, max(CHUNK_WIDTHS)), BF),
            pltpu.VMEM((2, BLOCKS, UNITS, max(CHUNK_WIDTHS)), BF),
            pltpu.VMEM((RING, RING, GROUP, META), BF),
            pltpu.VMEM((TOKENS, 128), F32),
            pltpu.SemaphoreType.DMA,
            pltpu.SemaphoreType.DMA((2, 2, 2)),
            pltpu.SemaphoreType.DMA((2, BLOCKS)),
            pltpu.SemaphoreType.DMA((10, GATHER_COPIES)),
            pltpu.SemaphoreType.DMA((10, GATHER_COPIES)),
        ],
        compiler_params=pltpu.CompilerParams(
            collective_id=0, has_side_effects=True, vmem_limit_bytes=60 * 1024 * 1024
        ),
        name="gather_rows",
    )(own, w_gate, w_up, w_down)


HALF = WIDTH // 2
WIDTHS = (384, 384, 256, 384, 256, 384)
STARTS = (0, 384, 768, 1024, 1408, 1664)
WIDEST = 384
STREAMS = 6
STREAM_COPIES = 22
AHEAD = (3, 1)
BEHIND = (2, 0)


def finish_kernel(grad_ref, hidden_ref, rows_ref, wg_ref, wu_ref, out_ref, dg_ref, du_ref, dd_ref, *scratch):
    n = STREAMS
    acc, mate, fa, ma, pa, fb, mb, pb, fc, mc, pc = [scratch[n * i : n * i + n] for i in range(11)]
    give, weights, done, other_done, across, tiles, made, some, wsem, tsem, msem, hsem, send, recv = scratch[11 * n :]
    plan = Plan(5.0, 9.0)
    at, core = place()
    partner = device(at, 1 - core)
    copies = {}
    every = pl.ds(0, RING)
    offset = (0, -1, 1, 2)

    def near(axis, by):
        return device(moved(at, axis, by), core)

    def coord(axis, by):
        return at[axis] if by == 0 else moved(at, axis, by)[axis]

    def spot(**over):
        to = {**at, **over}
        return to["z"], to["y"], to["x"]

    def order(s):
        return ORDERS[s % 3]

    def push(s, key, k, src, dst, peer, lane, count):
        copy = remote(src, dst, send.at[s, k], recv.at[s, k], peer)
        copy.start()
        copies[(s,) + key] = copy
        plan.send((s,) + key, lane, count * ROWS * WIDTHS[s] * 2)

    def along(s, key, k, src, dst, axis, by, count):
        push(s, key, k, src, dst, near(axis, by), (axis, by), count)

    turns = [(s, far) for c in (0, 3) for far in (True, False) for s in range(c, c + 3)]

    def fetch(turn):
        s, far = turns[turn]
        side = 1 - core if far else core
        columns = pl.ds(pl.multiple_of(side * HALF + STARTS[s], 128), WIDTHS[s])
        got = []
        for q in range(4):
            ref = (wg_ref, wu_ref)[q % 2].at[q // 2, :, columns]
            to = weights.at[turn % 2, q, :, pl.ds(0, WIDTHS[s])]
            got.append(pltpu.make_async_copy(ref, to, wsem.at[turn % 2, q]))
            got[-1].start()
        return got

    fetched = {0: fetch(0)}

    def compute(turn):
        s, far = turns[turn]
        w = WIDTHS[s]
        slot = turn % 2
        if turn + 1 < len(turns):
            fetched[turn + 1] = fetch(turn + 1)
        for copy in fetched[turn]:
            copy.wait()
        if far:
            if s >= 3:
                copies[s - 3, "far"].wait_send()
        else:
            copies[s, "far"].wait_recv()

        def rows_of(z, carry):
            take = pl.ds(pl.multiple_of(z * PLANE, 8), PLANE)
            total = jnp.dot(grad_ref[take, :UNITS], weights[slot, 0, :, :w], preferred_element_type=F32)
            for q in range(1, 4):
                total += jnp.dot(
                    grad_ref[take, q * UNITS : (q + 1) * UNITS], weights[slot, q, :, :w], preferred_element_type=F32
                )
            for i in range(RING * RING):
                y, x = i // RING, i % RING
                piece = total[i * ROWS : (i + 1) * ROWS]
                if far:
                    give[s % 3, z, y, x, :, :w] = piece.astype(BF)
                else:
                    acc[s][z, y, x] = (piece + mate[s][z, y, x].astype(F32)).astype(BF)
            return carry

        lax.fori_loop(0, RING, rows_of, 0)
        if far:
            push(s, ("far",), 21, give.at[s % 3, :, :, :, :, pl.ds(0, w)], mate[s], partner, "pair", 64)
        else:
            plan.mark(("own", s))

    def add(dst, index, *terms):
        total = dst[index].astype(F32)
        for ref, where in terms:
            total = total + ref[where].astype(F32)
        dst[index] = total.astype(BF)

    def line(s, r, by):
        d1, d2, d3 = order(s)
        return acc[s].at[spot(**{d1: every, d2: coord(d2, offset[r]), d3: coord(d3, by)})]

    def add_line(s, r, by, *terms, first=0, count=RING):
        d1, d2, d3 = order(s)

        def body(i, carry):
            where = spot(**{d1: i, d2: coord(d2, offset[r]), d3: coord(d3, by)})
            add(acc[s], where, *[(ref, (r, i) if lead else (i,)) for ref, lead in terms])
            return carry

        lax.fori_loop(first, first + count, body, 0)

    def piece(s, r, half):
        d1, d2, d3 = order(s)
        return acc[s].at[spot(**{d1: pl.ds(2 * half, 2), d2: coord(d2, offset[r])})]

    def half_of(ref, half):
        return ref.at[pl.ds(2 * half, 2)]

    def cell(s, by):
        d1 = order(s)[0]
        return spot(**{d1: coord(d1, by)})

    def travel(s):
        d1, d2, d3 = order(s)
        cost = 0.25
        yield [("own", s)], 0.1
        for up, down in ((3, 2), (1, 0)):
            yield [], 0.05, (d3, 1), (d3, -1)
            along(s, ("fa", up), up, line(s, up, 2), fa[s].at[up], d3, 1, 4)
            along(s, ("fa", down), down, line(s, down, 2), fa[s].at[down], d3, -1, 4)
        for up, down in ((2, 3), (0, 1)):
            yield [], 0.05, (d3, 1), (d3, -1)
            along(s, ("ma", up), 4 + up, line(s, up, 1), ma[s].at[up], d3, 1, 4)
            along(s, ("pa", down), 8 + down, line(s, down, -1), pa[s].at[down], d3, -1, 4)
        for r in (3, 2, 1, 0):
            yield [(s, "fa", r)], cost
            copies[s, "fa", r].wait_recv()
            if r in AHEAD:
                add_line(s, r, 1, (fa[s], True))
                along(s, ("ma", r), 4 + r, line(s, r, 1), ma[s].at[r], d3, 1, 4)
            else:
                add_line(s, r, -1, (fa[s], True))
                along(s, ("pa", r), 8 + r, line(s, r, -1), pa[s].at[r], d3, -1, 4)
        for r in (3, 2, 1, 0):
            yield [(s, "ma", r), (s, "pa", r)], cost
            copies[s, "ma", r].wait_recv()
            copies[s, "pa", r].wait_recv()
            add_line(s, r, 0, (ma[s], True), (pa[s], True))
            if r == 3:
                along(s, ("fb", 0), 12, piece(s, 3, 0), half_of(fb[s], 0), d2, 1, 2)
                along(s, ("fb", 1), 13, piece(s, 3, 1), half_of(fb[s], 1), d2, -1, 2)
            if r == 2:
                along(s, ("mb", 1), 15, piece(s, 2, 1), half_of(mb[s], 1), d2, 1, 2)
            if r == 1:
                along(s, ("pb", 0), 16, piece(s, 1, 0), half_of(pb[s], 0), d2, -1, 2)
        yield [(s, "fb", 0)], cost
        copies[s, "fb", 0].wait_recv()
        add_line(s, 2, 0, (fb[s], False), first=0, count=2)
        along(s, ("mb", 0), 14, piece(s, 2, 0), half_of(mb[s], 0), d2, 1, 2)
        yield [(s, "fb", 1)], cost
        copies[s, "fb", 1].wait_recv()
        add_line(s, 1, 0, (fb[s], False), first=2, count=2)
        along(s, ("pb", 1), 17, piece(s, 1, 1), half_of(pb[s], 1), d2, -1, 2)
        yield [(s, key, half) for key in ("mb", "pb") for half in (0, 1)], cost
        for half in (0, 1):
            copies[s, "mb", half].wait_recv()
            copies[s, "pb", half].wait_recv()
        add_line(s, 0, 0, (mb[s], False), (pb[s], False))
        along(s, ("fc",), 18, acc[s].at[cell(s, 2)], fc[s], d1, 1, 1)
        along(s, ("pc",), 20, acc[s].at[cell(s, -1)], pc[s], d1, -1, 1)
        yield [(s, "fc")], 0.1
        copies[s, "fc"].wait_recv()
        add(acc[s], cell(s, 1), (fc[s], ...))
        along(s, ("mc",), 19, acc[s].at[cell(s, 1)], mc[s], d1, 1, 1)
        yield [(s, "pc"), (s, "mc")], 0.1
        copies[s, "pc"].wait_recv()
        copies[s, "mc"].wait_recv()
        own = acc[s][cell(s, 0)].astype(F32) + pc[s][...].astype(F32) + mc[s][...].astype(F32)
        done[:, STARTS[s] : STARTS[s] + WIDTHS[s]] = own.astype(BF)
        plan.mark(("end", s))
        yield [("end", s)], 0.0

    def produce():
        for turn, (s, far) in enumerate(turns):
            yield [] if far else [(s, "far")], (1.9 if far else 2.8) * WIDTHS[s] / 384
            compute(turn)
        plan.mark("produced")

    def weigh():
        yield ["produced"], 0.2

        def load(t):
            got = []
            for a in range(2):
                src = rows_ref.at[a, :, pl.ds(META + t * UNITS, UNITS)]
                got.append(pltpu.make_async_copy(src, tiles.at[t % 2, a], tsem.at[t % 2, a]))
                got[-1].start()
            return got

        loaded = {0: load(0)}
        fetch_hidden = pltpu.make_async_copy(hidden_ref, some, hsem)
        fetch_hidden.start()
        for step in range(2):
            yield [], 2.2 if step == 0 else 1.2
            if step:
                fetch_hidden.wait()

            def turn_over(i, carry):
                where = pl.ds(pl.multiple_of(i * UNITS, UNITS), UNITS)
                for q in range(2 if step else 4):
                    src = (some if step else grad_ref)[where, q * UNITS : (q + 1) * UNITS]
                    across[4 * step + q, :, where] = src.T
                return carry

            lax.fori_loop(0, TOKENS // UNITS, turn_over, 0)
        stored = {}
        for t in range(WIDTH // UNITS):
            yield [], 2.0
            if t + 1 < WIDTH // UNITS:
                loaded[t + 1] = load(t + 1)
            for copy in loaded[t] + stored.pop(t - 2, []):
                copy.wait()

            def body(q, carry):
                value = jnp.dot(across[q], tiles[t % 2, q // 4], preferred_element_type=F32)
                made[t % 2, q] = value.astype(BF)
                return carry

            lax.fori_loop(0, BLOCKS, body, 0)
            stored[t] = []
            for q in range(BLOCKS):
                ref, j = ((dg_ref, du_ref)[q % 2], q // 2) if q < 4 else (dd_ref, q - 4)
                to = ref.at[j, :, pl.ds(t * UNITS, UNITS)]
                stored[t].append(pltpu.make_async_copy(made.at[t % 2, q], to, msem.at[t % 2, q]))
                stored[t][-1].start()
        for some_copies in stored.values():
            for copy in some_copies:
                copy.wait()

    greet(at, core)
    plan.run([travel(s) for s in range(n)] + [produce(), weigh()])
    last = remote(done, other_done, send.at[n, 0], recv.at[n, 0], partner)
    last.start()
    last.wait_recv()

    @pl.when(core == 0)
    def _():
        out_ref[:, :HALF] = done[0:20]
        out_ref[:, HALF:] = other_done[0:20]

    @pl.when(core == 1)
    def _():
        out_ref[:, :HALF] = other_done[20:40]
        out_ref[:, HALF:] = done[20:40]

    last.wait_send()
    for key, copy in copies.items():
        if key[1] != "far" or key[0] >= 3:
            copy.wait_send()


def finish(grads, hidden, rows, w_gate, w_up):
    full = [pltpu.VMEM((RING, RING, RING, ROWS, w), BF) for w in WIDTHS]
    lines = [pltpu.VMEM((RING, RING, ROWS, w), BF) for w in WIDTHS]
    line = [pltpu.VMEM((RING, ROWS, w), BF) for w in WIDTHS]
    cell = [pltpu.VMEM((ROWS, w), BF) for w in WIDTHS]
    anywhere = pl.BlockSpec(memory_space=pl.ANY)
    inside = pl.BlockSpec(memory_space=pltpu.VMEM)
    return pl.pallas_call(
        finish_kernel,
        out_shape=(jax.ShapeDtypeStruct((ROWS // 2, WIDTH), BF),) + (jax.ShapeDtypeStruct(w_gate.shape, BF),) * 3,
        in_specs=[inside] + [anywhere] * 4,
        out_specs=(inside,) + (anywhere,) * 3,
        scratch_shapes=full * 2
        + lines * 3
        + line * 3
        + cell * 3
        + [
            pltpu.VMEM((3, RING, RING, RING, ROWS, WIDEST), BF),
            pltpu.VMEM((2, 4, UNITS, WIDEST), BF),
            pltpu.VMEM((ROWS, HALF), BF),
            pltpu.VMEM((ROWS, HALF), BF),
            pltpu.VMEM((BLOCKS, UNITS, TOKENS), BF),
            pltpu.VMEM((2, 2, TOKENS, UNITS), BF),
            pltpu.VMEM((2, BLOCKS, UNITS, UNITS), BF),
            pltpu.VMEM((TOKENS, 2 * UNITS), BF),
            pltpu.SemaphoreType.DMA((2, 4)),
            pltpu.SemaphoreType.DMA((2, 2)),
            pltpu.SemaphoreType.DMA((2, BLOCKS)),
            pltpu.SemaphoreType.DMA,
            pltpu.SemaphoreType.DMA((STREAMS + 1, STREAM_COPIES)),
            pltpu.SemaphoreType.DMA((STREAMS + 1, STREAM_COPIES)),
        ],
        compiler_params=pltpu.CompilerParams(
            collective_id=1, has_side_effects=True, vmem_limit_bytes=67000000
        ),
        name="finish",
    )(grads, hidden, rows, w_gate, w_up)


def three(values):
    high = lax.reduce_precision(values, 8, 7)
    middle = lax.reduce_precision(values - high, 8, 7)
    return [high, middle, values - high - middle]


def own_rows(tokens, cotangent, routes, gate_weights, lengths, rewards):
    count = tokens.shape[0]
    wide = jnp.ones((count, 1), F32)
    columns = [routes.astype(F32)]
    for k in range(2):
        columns += three(gate_weights[:, k : k + 1])
    columns += [wide * lengths[0, 0].astype(F32), wide * rewards[0, 0].astype(F32)]
    meta = jnp.concatenate(columns, axis=1)
    meta = jnp.pad(meta, ((0, 0), (0, META - meta.shape[1]))).astype(BF)
    return jnp.stack(
        [jnp.concatenate([meta, tokens], axis=1), jnp.concatenate([jnp.zeros_like(meta), cotangent], axis=1)]
    )


def local(tokens, cotangent, routes, gate_weights, lengths, rewards, w_gate, w_up, w_down):
    own = own_rows(tokens, cotangent, routes, gate_weights, lengths, rewards)
    everything, grads, hidden = gather_rows(own, w_gate, w_up, w_down)
    everything = everything.reshape(2, TOKENS, WIDTH + META)
    return finish(grads, hidden, everything, w_gate, w_up)


def solution(mesh):
    rows = P(("dp", "expert", "sample"), None)
    pair = P(("dp", "expert"), "sample")
    weights = P("expert", ("dp", "sample"), None)
    return jax.shard_map(
        local,
        mesh=mesh,
        in_specs=(rows,) * 4 + (pair,) * 2 + (weights,) * 3,
        out_specs=(rows,) + (weights,) * 3,
        check_vma=False,
    )
```

```python
import jax
import jax.numpy as jnp
from jax import lax
from jax.experimental import pallas as pl
from jax.experimental.pallas import tpu as pltpu
from jax.sharding import PartitionSpec as P

RING = 4
WIDTH = 4096
META = 128
ROWS = 40
MESH = pl.DeviceIdType.MESH
ORDERS = (("x", "y", "z"), ("y", "z", "x"), ("z", "x", "y"))
BF = jnp.bfloat16
F32 = jnp.float32


def place():
    dp = lax.axis_index("dp")
    ex = lax.axis_index("expert")
    return {"x": lax.axis_index("sample"), "y": (dp % 2) * 2 + ex // 2, "z": dp // 2}, ex % 2


def device(at, core):
    return {
        "dp": at["z"] * 2 + at["y"] // 2,
        "expert": (at["y"] % 2) * 2 + core,
        "sample": at["x"],
    }


def moved(at, axis, by):
    return {**at, axis: lax.rem(at[axis] + (by + RING), RING)}


def greet(at, core):
    barrier = pltpu.get_barrier_semaphore()
    peers = [device(moved(at, axis, by), core) for axis in "xyz" for by in (1, -1)]
    peers.append(device(at, 1 - core))
    for peer in peers:
        pl.semaphore_signal(barrier, inc=1, device_id=peer, device_id_type=MESH)
    pl.semaphore_wait(barrier, len(peers))


def remote(src, dst, send, recv, peer):
    return pltpu.make_async_remote_copy(
        src_ref=src, dst_ref=dst, send_sem=send, recv_sem=recv, device_id=peer, device_id_type=MESH
    )


class Plan:
    def __init__(self, delay, slack):
        self.delay = delay
        self.slack = slack
        self.now = 0.0
        self.free = {}
        self.ready = {}

    def send(self, key, lane, size):
        rate, delay = (5e5, 1.5) if lane == "pair" else (4.6e4, self.delay)
        end = max(self.now, self.free.get(lane, 0.0)) + size / rate
        self.free[lane] = end
        self.ready[key] = end + delay

    def mark(self, key, delay=0.0):
        self.ready[key] = self.now + delay

    def run(self, actors):
        waiting = [(actor, next(actor, None)) for actor in actors]
        while any(need is not None for _, need in waiting):
            best = None
            for i, (actor, need) in enumerate(waiting):
                if need is None or any(key not in self.ready for key in need[0]):
                    continue
                queued = [self.free.get(lane, 0.0) - self.slack for lane in need[2:]]
                at = max([self.now] + [self.ready[key] for key in need[0]] + queued)
                if best is None or at < best[0]:
                    best = (at, i)
            at, i = best
            actor, need = waiting[i]
            self.now = at + need[1]
            waiting[i] = (actor, next(actor, None))


CHUNK_WIDTHS = (256, 640, 512)
CHUNK_STARTS = (0, 256, 896)
PART = (WIDTH + META) // 3
GATHER_COPIES = 23
GROUP = RING * ROWS
TOKENS = RING * RING * GROUP
PLANE = RING * GROUP
UNITS = 256
BLOCKS = 6


def turned(a, b):
    return lax.dot_general(a, b, (((1,), (1,)), ((), ())), preferred_element_type=F32)


def gather_kernel(own_ref, wg_ref, wu_ref, wd_ref, out_ref, grad_ref, hidden_ref, *scratch):
    mate, block, total, tiles, weights, info, scales, keep, tsem, wsem, send, recv = scratch
    at, core = place()
    partner = device(at, 1 - core)
    plan = Plan(3.4, 5.0)
    copies = {}
    settled = []
    greet(at, core)
    swap = remote(own_ref.at[1 - core], mate, send.at[9, 0], recv.at[9, 0], partner)
    swap.start()
    swap.wait()

    @pl.when(core == 0)
    def _():
        block[0:20] = own_ref[0]
        block[20:40] = mate[...]

    @pl.when(core == 1)
    def _():
        block[0:20] = mate[...]
        block[20:40] = own_ref[1]

    here = pltpu.make_async_copy(block, out_ref.at[core, at["z"], at["y"], pl.ds(pl.multiple_of(at["x"] * ROWS, 8), ROWS)], keep)
    here.start()

    def columns(s):
        return pl.ds((s % 3) * PART + CHUNK_STARTS[s // 3], CHUNK_WIDTHS[s // 3])

    def view(s, **over):
        to = {**at, **over}
        x = to["x"]
        if isinstance(x, pl.Slice):
            x = pl.ds(x.start * ROWS, x.size * ROWS)
        else:
            x = pl.ds(pl.multiple_of(x * ROWS, 8), ROWS)
        return out_ref.at[core, to["z"], to["y"], x, columns(s)]

    def push(s, k, src, dst, peer, lane, count):
        copy = remote(src, dst, send.at[s, k], recv.at[s, k], peer)
        copy.start()
        copies[s, k] = copy
        plan.send((s, k), lane, count * ROWS * CHUNK_WIDTHS[s // 3] * 2)

    def near(axis, by):
        return device(moved(at, axis, by), core)

    def coord(axis, by):
        return at[axis] if by == 0 else moved(at, axis, by)[axis]

    every = pl.ds(0, RING)
    offset = (0, -1, 1, 2)

    def line(s, l, plane=0):
        d1, d2, d3 = ORDERS[s % 3]
        return view(s, **{d1: every, d2: coord(d2, offset[l]), d3: coord(d3, plane)})

    def hand(s, n):
        d1, d2, d3 = ORDERS[s % 3]
        ref = view(s, **{d1: every, d2: every, d3: coord(d3, offset[n])})
        push(s, 19 + n, ref, ref, partner, "pair", 16)

    def travel(s):
        d1, d2, d3 = ORDERS[s % 3]
        tick = 0.05

        def along(k, ref, axis, by, count):
            push(s, k, ref, ref, near(axis, by), (axis, by), count)

        def spread(l):
            along(7 + 2 * l, line(s, l), d3, 1, 4)
            along(8 + 2 * l, line(s, l), d3, -1, 4)

        mine = block.at[:, columns(s)]
        for k, by in ((0, 1), (1, -1)):
            push(s, k, mine, view(s), near(d1, by), (d1, by), 1)
        ahead = lambda *axes: [(axis, by) for axis in axes for by in (1, -1)] if s >= 3 else []
        yield [(s, 0)], tick, *ahead(d1)
        copies[s, 0].wait_recv()
        along(2, view(s, **{d1: coord(d1, -1)}), d1, 1, 1)
        yield [(s, 1), (s, 2)], tick, *ahead(d2)
        copies[s, 1].wait_recv()
        copies[s, 2].wait_recv()
        if not settled:
            here.wait()
            settled.append(True)
        along(3, line(s, 0), d2, 1, 4)
        along(4, line(s, 0), d2, -1, 4)
        yield [], tick, (d3, 1), (d3, -1)
        spread(0)
        yield [(s, 3)], tick
        copies[s, 3].wait_recv()
        along(5, view(s, **{d1: pl.ds(0, 2), d2: coord(d2, -1)}), d2, 1, 2)
        yield [(s, 4)], tick
        copies[s, 4].wait_recv()
        along(6, view(s, **{d1: pl.ds(2, 2), d2: coord(d2, 1)}), d2, -1, 2)
        for l in (1, 2):
            yield [], tick, (d3, 1), (d3, -1)
            spread(l)
        yield [(s, 5), (s, 6)], tick
        copies[s, 5].wait_recv()
        copies[s, 6].wait_recv()
        spread(3)
        hand(s, 0)
        for l in range(4):
            for k, by in ((0, 1), (1, -1)):
                yield [(s, 7 + 2 * l + k)], tick
                copies[s, 7 + 2 * l + k].wait_recv()
                if k == l // 2:
                    along(15 + l, line(s, l, -by), d3, by, 4)
        hand(s, 1)
        hand(s, 2)
        yield [(s, 15 + l) for l in range(4)], tick
        for l in range(4):
            copies[s, 15 + l].wait_recv()
        hand(s, 3)
        plan.mark(("all", s))

    first = (2 * lax.axis_index("expert")).astype(F32)
    same = (
        lax.broadcasted_iota(jnp.int32, (GROUP, GROUP), 0) % ROWS
        == lax.broadcasted_iota(jnp.int32, (GROUP, GROUP), 1) % ROWS
    ).astype(F32).astype(BF)

    def scale(i, carry):
        rows = info[i // RING, i % RING]
        meta = rows.astype(F32)
        reward = meta[:, 9:10] * 0.0625
        all_rewards = jnp.dot(same, rows, preferred_element_type=F32)[:, 9:10] * 0.0625
        advantage = reward - (all_rewards - reward) / 3.0
        position = lax.broadcasted_iota(jnp.int32, (GROUP, 1), 0) % 20
        weight = jnp.where(position.astype(F32) < meta[:, 8:9], -advantage, 0.0)
        lane = lax.broadcasted_iota(jnp.int32, (GROUP, 128), 1).astype(F32)
        value = jnp.zeros((GROUP, 128), F32)
        for k in range(2):
            c = 2 + 3 * k
            pair = ((meta[:, c : c + 1] + meta[:, c + 1 : c + 2]) + meta[:, c + 2 : c + 3]) * weight
            value = jnp.where(lane == meta[:, k : k + 1] - first, pair, value)
        scales[pl.ds(pl.multiple_of(i * GROUP, 8), GROUP), :] = value
        return carry

    pending = {}

    def needs(s):
        return [("all", s)] + [(s, 19 + n) for n in range(4)]

    def begin(s):
        w = CHUNK_WIDTHS[s // 3]
        for n in range(4):
            copies[s, 19 + n].wait_recv()
        lead = META if s == 0 else 0
        start = (s % 3) * PART + CHUNK_STARTS[s // 3] - META + lead
        slot = s % 2
        loads = [[], []]
        sources = ((wg_ref, 0), (wu_ref, 0), (wg_ref, 1), (wu_ref, 1), (wd_ref, 0), (wd_ref, 1))
        for k, (ref, j) in enumerate(sources):
            to = weights.at[slot, k, :, pl.ds(lead, w - lead)]
            loads[0].append(pltpu.make_async_copy(ref.at[j, :, pl.ds(start, w - lead)], to, wsem.at[slot, k]))
        for half in range(2):
            for a in range(2):
                src = out_ref.at[a, pl.ds(2 * half, 2), :, :, columns(s)]
                to = tiles.at[slot, half, a, :, :, :, pl.ds(0, w)]
                loads[half].append(pltpu.make_async_copy(src, to, tsem.at[slot, half, a]))
        if s == 0:
            loads[0].append(pltpu.make_async_copy(out_ref.at[0, :, :, :, pl.ds(0, META)], info, keep))
            weights[0, :, :, :META] = jnp.zeros((BLOCKS, UNITS, META), BF)
        for half in range(2):
            for copy in loads[half]:
                copy.start()
        pending[s] = loads
        plan.mark(("load", s), 2.5)

    def work():
        for s in range(9):
            w = CHUNK_WIDTHS[s // 3]
            cost = {640: 2.7, 512: 2.2, 384: 2.0, 256: 1.7}[w]
            if s not in pending:
                yield needs(s), 0.1
                begin(s)
            for half in range(2):
                yield [("load", s)], cost
                for copy in pending[s][half]:
                    copy.wait()

                def body(i, carry):
                    z, pair = i // 3, i % 3
                    tile = tiles[s % 2, half, pair // 2, z, :, :, :w].reshape(PLANE, w)
                    where = pl.ds(pl.multiple_of((2 * half + z) * PLANE, 8), PLANE)
                    for k in range(2):
                        q = pair * 2 + k
                        value = turned(tile, weights[s % 2, q, :, :w])
                        if s == 0:
                            total[q, where, :] = value
                        else:
                            total[q, where, :] += value
                    return carry

                lax.fori_loop(0, 6, body, 0)
                if half == 0 and s < 8 and all(plan.ready.get(key, 1e9) <= plan.now for key in needs(s + 1)):
                    begin(s + 1)
            if s == 0:
                yield [], 4.2
                lax.fori_loop(0, RING * RING, scale, 0)

    plan.run([travel(s) for s in range(9)] + [work()])

    def activate(i, carry):
        where = pl.ds(pl.multiple_of(i * 128, 128), 128)
        for j in range(2):
            pre_gate, pre_up = total[2 * j, where, :], total[2 * j + 1, where, :]
            by = scales[where, j : j + 1]
            grad_hidden = total[4 + j, where, :] * by
            prob = 1.0 / (1.0 + jnp.exp(-pre_gate))
            active = pre_gate * prob
            slope = prob * (1.0 + pre_gate * (1.0 - prob))
            grad_ref[where, 2 * j * UNITS : (2 * j + 1) * UNITS] = (grad_hidden * pre_up * slope).astype(BF)
            grad_ref[where, (2 * j + 1) * UNITS : (2 * j + 2) * UNITS] = (grad_hidden * active).astype(BF)
            hidden_ref[where, j * UNITS : (j + 1) * UNITS] = (active * pre_up * by).astype(BF)
        return carry

    lax.fori_loop(0, TOKENS // 128, activate, 0)
    for copy in copies.values():
        copy.wait_send()


def gather_rows(own, w_gate, w_up, w_down):
    anywhere = pl.BlockSpec(memory_space=pl.ANY)
    inside = pl.BlockSpec(memory_space=pltpu.VMEM)
    return pl.pallas_call(
        gather_kernel,
        out_shape=(
            jax.ShapeDtypeStruct((2, RING, RING, GROUP, WIDTH + META), BF),
            jax.ShapeDtypeStruct((TOKENS, 4 * UNITS), BF),
            jax.ShapeDtypeStruct((TOKENS, 2 * UNITS), BF),
        ),
        in_specs=[inside] + [anywhere] * 3,
        out_specs=(anywhere, inside, inside),
        scratch_shapes=[
            pltpu.VMEM((ROWS // 2, WIDTH + META), BF),
            pltpu.VMEM((ROWS, WIDTH + META), BF),
            pltpu.VMEM((BLOCKS, TOKENS, UNITS), F32),
            pltpu.VMEM((2, 2, 2, 2, RING, GROUP, max(CHUNK_WIDTHS)), BF),
            pltpu.VMEM((2, BLOCKS, UNITS, max(CHUNK_WIDTHS)), BF),
            pltpu.VMEM((RING, RING, GROUP, META), BF),
            pltpu.VMEM((TOKENS, 128), F32),
            pltpu.SemaphoreType.DMA,
            pltpu.SemaphoreType.DMA((2, 2, 2)),
            pltpu.SemaphoreType.DMA((2, BLOCKS)),
            pltpu.SemaphoreType.DMA((10, GATHER_COPIES)),
            pltpu.SemaphoreType.DMA((10, GATHER_COPIES)),
        ],
        compiler_params=pltpu.CompilerParams(
            collective_id=0, has_side_effects=True, vmem_limit_bytes=60 * 1024 * 1024
        ),
        name="gather_rows",
    )(own, w_gate, w_up, w_down)


HALF = WIDTH // 2
WIDTHS = (384, 384, 256, 384, 256, 384)
STARTS = (0, 384, 768, 1024, 1408, 1664)
WIDEST = 384
STREAMS = 6
STREAM_COPIES = 22
AHEAD = (3, 1)
BEHIND = (2, 0)


def finish_kernel(grad_ref, hidden_ref, rows_ref, wg_ref, wu_ref, out_ref, dg_ref, du_ref, dd_ref, *scratch):
    n = STREAMS
    acc, mate, fa, ma, pa, fb, mb, pb, fc, mc, pc = [scratch[n * i : n * i + n] for i in range(11)]
    give, weights, done, other_done, across, tiles, made, some, wsem, tsem, msem, hsem, send, recv = scratch[11 * n :]
    plan = Plan(5.0, 9.0)
    at, core = place()
    partner = device(at, 1 - core)
    copies = {}
    every = pl.ds(0, RING)
    offset = (0, -1, 1, 2)

    def near(axis, by):
        return device(moved(at, axis, by), core)

    def coord(axis, by):
        return at[axis] if by == 0 else moved(at, axis, by)[axis]

    def spot(**over):
        to = {**at, **over}
        return to["z"], to["y"], to["x"]

    def order(s):
        return ORDERS[s % 3]

    def push(s, key, k, src, dst, peer, lane, count):
        copy = remote(src, dst, send.at[s, k], recv.at[s, k], peer)
        copy.start()
        copies[(s,) + key] = copy
        plan.send((s,) + key, lane, count * ROWS * WIDTHS[s] * 2)

    def along(s, key, k, src, dst, axis, by, count):
        push(s, key, k, src, dst, near(axis, by), (axis, by), count)

    turns = [(s, far) for c in (0, 3) for far in (True, False) for s in range(c, c + 3)]

    def fetch(turn):
        s, far = turns[turn]
        side = 1 - core if far else core
        columns = pl.ds(pl.multiple_of(side * HALF + STARTS[s], 128), WIDTHS[s])
        got = []
        for q in range(4):
            ref = (wg_ref, wu_ref)[q % 2].at[q // 2, :, columns]
            to = weights.at[turn % 2, q, :, pl.ds(0, WIDTHS[s])]
            got.append(pltpu.make_async_copy(ref, to, wsem.at[turn % 2, q]))
            got[-1].start()
        return got

    fetched = {0: fetch(0)}

    def compute(turn):
        s, far = turns[turn]
        w = WIDTHS[s]
        slot = turn % 2
        if turn + 1 < len(turns):
            fetched[turn + 1] = fetch(turn + 1)
        for copy in fetched[turn]:
            copy.wait()
        if far:
            if s >= 3:
                copies[s - 3, "far"].wait_send()
        else:
            copies[s, "far"].wait_recv()

        def rows_of(z, carry):
            take = pl.ds(pl.multiple_of(z * PLANE, 8), PLANE)
            total = jnp.dot(grad_ref[take, :UNITS], weights[slot, 0, :, :w], preferred_element_type=F32)
            for q in range(1, 4):
                total += jnp.dot(
                    grad_ref[take, q * UNITS : (q + 1) * UNITS], weights[slot, q, :, :w], preferred_element_type=F32
                )
            for i in range(RING * RING):
                y, x = i // RING, i % RING
                piece = total[i * ROWS : (i + 1) * ROWS]
                if far:
                    give[s % 3, z, y, x, :, :w] = piece.astype(BF)
                else:
                    acc[s][z, y, x] = (piece + mate[s][z, y, x].astype(F32)).astype(BF)
            return carry

        lax.fori_loop(0, RING, rows_of, 0)
        if far:
            push(s, ("far",), 21, give.at[s % 3, :, :, :, :, pl.ds(0, w)], mate[s], partner, "pair", 64)
        else:
            plan.mark(("own", s))

    def add(dst, index, *terms):
        total = dst[index].astype(F32)
        for ref, where in terms:
            total = total + ref[where].astype(F32)
        dst[index] = total.astype(BF)

    def line(s, r, by):
        d1, d2, d3 = order(s)
        return acc[s].at[spot(**{d1: every, d2: coord(d2, offset[r]), d3: coord(d3, by)})]

    def add_line(s, r, by, *terms, first=0, count=RING):
        d1, d2, d3 = order(s)

        def body(i, carry):
            where = spot(**{d1: i, d2: coord(d2, offset[r]), d3: coord(d3, by)})
            add(acc[s], where, *[(ref, (r, i) if lead else (i,)) for ref, lead in terms])
            return carry

        lax.fori_loop(first, first + count, body, 0)

    def piece(s, r, half):
        d1, d2, d3 = order(s)
        return acc[s].at[spot(**{d1: pl.ds(2 * half, 2), d2: coord(d2, offset[r])})]

    def half_of(ref, half):
        return ref.at[pl.ds(2 * half, 2)]

    def cell(s, by):
        d1 = order(s)[0]
        return spot(**{d1: coord(d1, by)})

    def travel(s):
        d1, d2, d3 = order(s)
        cost = 0.25
        yield [("own", s)], 0.1
        for up, down in ((3, 2), (1, 0)):
            yield [], 0.05, (d3, 1), (d3, -1)
            along(s, ("fa", up), up, line(s, up, 2), fa[s].at[up], d3, 1, 4)
            along(s, ("fa", down), down, line(s, down, 2), fa[s].at[down], d3, -1, 4)
        for up, down in ((2, 3), (0, 1)):
            yield [], 0.05, (d3, 1), (d3, -1)
            along(s, ("ma", up), 4 + up, line(s, up, 1), ma[s].at[up], d3, 1, 4)
            along(s, ("pa", down), 8 + down, line(s, down, -1), pa[s].at[down], d3, -1, 4)
        for r in (3, 2, 1, 0):
            yield [(s, "fa", r)], cost
            copies[s, "fa", r].wait_recv()
            if r in AHEAD:
                add_line(s, r, 1, (fa[s], True))
                along(s, ("ma", r), 4 + r, line(s, r, 1), ma[s].at[r], d3, 1, 4)
            else:
                add_line(s, r, -1, (fa[s], True))
                along(s, ("pa", r), 8 + r, line(s, r, -1), pa[s].at[r], d3, -1, 4)
        for r in (3, 2, 1, 0):
            yield [(s, "ma", r), (s, "pa", r)], cost
            copies[s, "ma", r].wait_recv()
            copies[s, "pa", r].wait_recv()
            add_line(s, r, 0, (ma[s], True), (pa[s], True))
            if r == 3:
                along(s, ("fb", 0), 12, piece(s, 3, 0), half_of(fb[s], 0), d2, 1, 2)
                along(s, ("fb", 1), 13, piece(s, 3, 1), half_of(fb[s], 1), d2, -1, 2)
            if r == 2:
                along(s, ("mb", 1), 15, piece(s, 2, 1), half_of(mb[s], 1), d2, 1, 2)
            if r == 1:
                along(s, ("pb", 0), 16, piece(s, 1, 0), half_of(pb[s], 0), d2, -1, 2)
        yield [(s, "fb", 0)], cost
        copies[s, "fb", 0].wait_recv()
        add_line(s, 2, 0, (fb[s], False), first=0, count=2)
        along(s, ("mb", 0), 14, piece(s, 2, 0), half_of(mb[s], 0), d2, 1, 2)
        yield [(s, "fb", 1)], cost
        copies[s, "fb", 1].wait_recv()
        add_line(s, 1, 0, (fb[s], False), first=2, count=2)
        along(s, ("pb", 1), 17, piece(s, 1, 1), half_of(pb[s], 1), d2, -1, 2)
        yield [(s, key, half) for key in ("mb", "pb") for half in (0, 1)], cost
        for half in (0, 1):
            copies[s, "mb", half].wait_recv()
            copies[s, "pb", half].wait_recv()
        add_line(s, 0, 0, (mb[s], False), (pb[s], False))
        along(s, ("fc",), 18, acc[s].at[cell(s, 2)], fc[s], d1, 1, 1)
        along(s, ("pc",), 20, acc[s].at[cell(s, -1)], pc[s], d1, -1, 1)
        yield [(s, "fc")], 0.1
        copies[s, "fc"].wait_recv()
        add(acc[s], cell(s, 1), (fc[s], ...))
        along(s, ("mc",), 19, acc[s].at[cell(s, 1)], mc[s], d1, 1, 1)
        yield [(s, "pc"), (s, "mc")], 0.1
        copies[s, "pc"].wait_recv()
        copies[s, "mc"].wait_recv()
        own = acc[s][cell(s, 0)].astype(F32) + pc[s][...].astype(F32) + mc[s][...].astype(F32)
        done[:, STARTS[s] : STARTS[s] + WIDTHS[s]] = own.astype(BF)
        plan.mark(("end", s))
        yield [("end", s)], 0.0

    def produce():
        for turn, (s, far) in enumerate(turns):
            yield [] if far else [(s, "far")], (1.9 if far else 2.8) * WIDTHS[s] / 384
            compute(turn)
        plan.mark("produced")

    def weigh():
        yield ["produced"], 0.2

        def load(t):
            got = []
            for a in range(2):
                src = rows_ref.at[a, :, pl.ds(META + t * UNITS, UNITS)]
                got.append(pltpu.make_async_copy(src, tiles.at[t % 2, a], tsem.at[t % 2, a]))
                got[-1].start()
            return got

        loaded = {0: load(0)}
        fetch_hidden = pltpu.make_async_copy(hidden_ref, some, hsem)
        fetch_hidden.start()
        for step in range(2):
            yield [], 2.2 if step == 0 else 1.2
            if step:
                fetch_hidden.wait()

            def turn_over(i, carry):
                where = pl.ds(pl.multiple_of(i * UNITS, UNITS), UNITS)
                for q in range(2 if step else 4):
                    src = (some if step else grad_ref)[where, q * UNITS : (q + 1) * UNITS]
                    across[4 * step + q, :, where] = src.T
                return carry

            lax.fori_loop(0, TOKENS // UNITS, turn_over, 0)
        stored = {}
        for t in range(WIDTH // UNITS):
            yield [], 2.0
            if t + 1 < WIDTH // UNITS:
                loaded[t + 1] = load(t + 1)
            for copy in loaded[t] + stored.pop(t - 2, []):
                copy.wait()

            def body(q, carry):
                value = jnp.dot(across[q], tiles[t % 2, q // 4], preferred_element_type=F32)
                made[t % 2, q] = value.astype(BF)
                return carry

            lax.fori_loop(0, BLOCKS, body, 0)
            stored[t] = []
            for q in range(BLOCKS):
                ref, j = ((dg_ref, du_ref)[q % 2], q // 2) if q < 4 else (dd_ref, q - 4)
                to = ref.at[j, :, pl.ds(t * UNITS, UNITS)]
                stored[t].append(pltpu.make_async_copy(made.at[t % 2, q], to, msem.at[t % 2, q]))
                stored[t][-1].start()
        for some_copies in stored.values():
            for copy in some_copies:
                copy.wait()

    greet(at, core)
    plan.run([travel(s) for s in range(n)] + [produce(), weigh()])
    last = remote(done, other_done, send.at[n, 0], recv.at[n, 0], partner)
    last.start()
    last.wait_recv()

    @pl.when(core == 0)
    def _():
        out_ref[:, :HALF] = done[0:20]
        out_ref[:, HALF:] = other_done[0:20]

    @pl.when(core == 1)
    def _():
        out_ref[:, :HALF] = other_done[20:40]
        out_ref[:, HALF:] = done[20:40]

    last.wait_send()
    for key, copy in copies.items():
        if key[1] != "far" or key[0] >= 3:
            copy.wait_send()


def finish(grads, hidden, rows, w_gate, w_up):
    full = [pltpu.VMEM((RING, RING, RING, ROWS, w), BF) for w in WIDTHS]
    lines = [pltpu.VMEM((RING, RING, ROWS, w), BF) for w in WIDTHS]
    line = [pltpu.VMEM((RING, ROWS, w), BF) for w in WIDTHS]
    cell = [pltpu.VMEM((ROWS, w), BF) for w in WIDTHS]
    anywhere = pl.BlockSpec(memory_space=pl.ANY)
    inside = pl.BlockSpec(memory_space=pltpu.VMEM)
    return pl.pallas_call(
        finish_kernel,
        out_shape=(jax.ShapeDtypeStruct((ROWS // 2, WIDTH), BF),) + (jax.ShapeDtypeStruct(w_gate.shape, BF),) * 3,
        in_specs=[inside] + [anywhere] * 4,
        out_specs=(inside,) + (anywhere,) * 3,
        scratch_shapes=full * 2
        + lines * 3
        + line * 3
        + cell * 3
        + [
            pltpu.VMEM((3, RING, RING, RING, ROWS, WIDEST), BF),
            pltpu.VMEM((2, 4, UNITS, WIDEST), BF),
            pltpu.VMEM((ROWS, HALF), BF),
            pltpu.VMEM((ROWS, HALF), BF),
            pltpu.VMEM((BLOCKS, UNITS, TOKENS), BF),
            pltpu.VMEM((2, 2, TOKENS, UNITS), BF),
            pltpu.VMEM((2, BLOCKS, UNITS, UNITS), BF),
            pltpu.VMEM((TOKENS, 2 * UNITS), BF),
            pltpu.SemaphoreType.DMA((2, 4)),
            pltpu.SemaphoreType.DMA((2, 2)),
            pltpu.SemaphoreType.DMA((2, BLOCKS)),
            pltpu.SemaphoreType.DMA,
            pltpu.SemaphoreType.DMA((STREAMS + 1, STREAM_COPIES)),
            pltpu.SemaphoreType.DMA((STREAMS + 1, STREAM_COPIES)),
        ],
        compiler_params=pltpu.CompilerParams(
            collective_id=1, has_side_effects=True, vmem_limit_bytes=67000000
        ),
        name="finish",
    )(grads, hidden, rows, w_gate, w_up)


def three(values):
    high = lax.reduce_precision(values, 8, 7)
    middle = lax.reduce_precision(values - high, 8, 7)
    return [high, middle, values - high - middle]


def own_rows(tokens, cotangent, routes, gate_weights, lengths, rewards):
    count = tokens.shape[0]
    wide = jnp.ones((count, 1), F32)
    columns = [routes.astype(F32)]
    for k in range(2):
        columns += three(gate_weights[:, k : k + 1])
    columns += [wide * lengths[0, 0].astype(F32), wide * rewards[0, 0].astype(F32)]
    meta = jnp.concatenate(columns, axis=1)
    meta = jnp.pad(meta, ((0, 0), (0, META - meta.shape[1]))).astype(BF)
    return jnp.stack(
        [jnp.concatenate([meta, tokens], axis=1), jnp.concatenate([jnp.zeros_like(meta), cotangent], axis=1)]
    )


def local(tokens, cotangent, routes, gate_weights, lengths, rewards, w_gate, w_up, w_down):
    own = own_rows(tokens, cotangent, routes, gate_weights, lengths, rewards)
    everything, grads, hidden = gather_rows(own, w_gate, w_up, w_down)
    everything = everything.reshape(2, TOKENS, WIDTH + META)
    return finish(grads, hidden, everything, w_gate, w_up)


def solution(mesh):
    rows = P(("dp", "expert", "sample"), None)
    pair = P(("dp", "expert"), "sample")
    weights = P("expert", ("dp", "sample"), None)
    return jax.shard_map(
        local,
        mesh=mesh,
        in_specs=(rows,) * 4 + (pair,) * 2 + (weights,) * 3,
        out_specs=(rows,) + (weights,) * 3,
        check_vma=False,
    )
```
